32 devices in a mesh: vocab: 8 (over z, y), dp: 4 (over x, core).
Axes of the slice: x: 2, y: 2, z: 4, core: 2. Of those that a mesh axis runs over, the one named last changes fastest.
Arguments:
- hidden: bfloat16 [4096, 4096], P('dp'), may hold values from -6 to 6
- labels: int32 [4096], P('dp'), may hold values from 0 to 3, as said below
- targets: int32 [4096], P('dp'), may hold values from 0 to 147455, as said below
- head_weight: bfloat16 [4096, 16384], P(None, 'vocab'), may hold values from -0.125 to 0.125
- cluster_weight: bfloat16 [4096, 3], replicated, may hold values from -0.09375 to 0.09375
- proj_one: bfloat16 [4096, 1024], P('vocab'), may hold values from -0.09375 to 0.09375
- proj_two: bfloat16 [4096, 256], P('vocab'), may hold values from -0.09375 to 0.09375
- proj_three: bfloat16 [4096, 64], P('vocab'), may hold values from -0.09375 to 0.09375
- out_one: bfloat16 [1024, 32768], P(None, 'vocab'), may hold values from -0.1875 to 0.1875
- out_two: bfloat16 [256, 65536], P(None, 'vocab'), may hold values from -0.375 to 0.375
- out_three: bfloat16 [64, 147456], P(None, 'vocab'), may hold values from -0.75 to 0.75
Outputs:
- token_loss: float32 [4096], P('dp')
- mean_loss: float32 [], replicated
- hidden_grad: float32 [4096, 4096], P('dp', 'vocab')
The draws below stay inside these ranges and needn't reach their ends.
Inputs may be any that keep to these rules, and one draw needn't show every extreme that they name: In each aligned block of 1024 tokens (one index of dp), each of the labels 1, 2 and 3 marks at most 256 tokens and at least 128; for each label some block holds exactly 256 of them. `targets`: A token's target is below 16384 if its label is 0, below 32768, 65536 or 147456 if its label is 1, 2 or 3.
All inputs are finite; a program needn't handle non-finite values.
Results may differ from the reference program's by a relative error of at most 0.0013.
Values sent between devices are 32-bit elements; how exact they have to be, the bound alone decides.
A program may use at most 128 MiB of HBM per device.

```python
import jax
import jax.numpy as jnp
from jax import lax

D = 4096
HEAD = 16384
P1 = 1024
P2 = 256
P3 = 64
V1 = 32768
V2 = 65536
V3 = 147456
GRP_TOK = 1024
CAP = 256
TOKENS = 4096


def label_parts(key):
    groups = TOKENS // GRP_TOK
    first_key, second_key, third_key, fourth_key = jax.random.split(jax.random.fold_in(key, 17), 4)
    full_group = jax.random.randint(first_key, (3,), 0, groups)
    amounts = jax.random.randint(second_key, (groups, 3), CAP // 2, CAP + 1)
    amounts = jnp.where(jnp.arange(groups)[:, None] == full_group[None, :], CAP, amounts).astype(jnp.int32)
    edges = jnp.cumsum(amounts, axis=1)
    places = jnp.arange(GRP_TOK, dtype=jnp.int32)[None, :]
    sorted_labels = jnp.where(places < edges[:, 0:1], 1, jnp.where(places < edges[:, 1:2], 2, jnp.where(places < edges[:, 2:3], 3, 0)))
    shuffles = jax.vmap(lambda sub_key: jax.random.permutation(sub_key, GRP_TOK))(jax.random.split(third_key, groups))
    labels = jnp.take_along_axis(sorted_labels, shuffles, axis=1).reshape(TOKENS).astype(jnp.int32)
    limits = jnp.array([HEAD, V1, V2, V3], jnp.int32)[labels]
    raw_ids = jax.random.randint(fourth_key, (TOKENS,), 0, 2 ** 30, dtype=jnp.int32)
    targets = (raw_ids % limits).astype(jnp.int32)
    return (labels, targets)


def draw_labels(key, part):
    return label_parts(key)[0]


def draw_targets(key, part):
    return label_parts(key)[1]


def raised(values, own_key, source, target, shards_of, factor):
    owner, partner = [(jnp.arange(values.shape[axis_at]) // (values.shape[axis_at] // shards_of)).reshape([-1 if axis == axis_at else 1 for axis in range(values.ndim)]) for axis_at in (source, target)]
    chosen = jax.random.permutation(own_key, shards_of)[partner]
    strong = (owner == chosen) | (owner == (partner + shards_of // 2) % shards_of)
    return jnp.where(strong, factor * values, values)


def levels(key, extent, pieces, smallest, largest):
    loudness = 1.0
    for position, shards_of in pieces:
        steps = jax.random.uniform(jax.random.fold_in(jax.random.fold_in(key, 6), position), (shards_of,), jnp.float32, smallest / len(pieces), largest / len(pieces))
        loudness = loudness * jnp.repeat(jnp.exp(steps), extent[position] // shards_of).reshape((-1,) + (1,) * (len(extent) - 1 - position))
    return loudness


def gaussian(key, extent, deviation, most, cuts=(), kind=jnp.bfloat16):
    factor_of = levels(key, extent, cuts, -0.22, 0.18) if cuts else 1.0
    values = jax.random.normal(key, extent, jnp.float32) * deviation * factor_of
    return jnp.minimum(jnp.maximum(values, -most), most).astype(kind)


def bell_draw_with(key, extent, width, reach, shards, heavy, kind=jnp.bfloat16):
    values = width * jax.random.normal(key, extent, jnp.float32)
    if shards:
        values = values * levels(key, extent, shards, -0.22, 0.18)
    return jnp.clip(raised(values, jax.random.fold_in(key, 3), *heavy), -reach, reach).astype(kind)


def setup_inputs(seed: int = 0) -> dict:
    streams_of = jax.random.split(jax.random.key(seed), 12)
    hidden = gaussian(streams_of[0], (TOKENS, D), 1.0, 6.0, ((0, 4),))
    labels = draw_labels(jax.random.fold_in(streams_of[11], 71), 0)
    targets = draw_targets(jax.random.fold_in(streams_of[11], 71), 0)
    head_weight = bell_draw_with(streams_of[3], (D, HEAD), D ** -0.5, 0.125, ((1, 8),), (1, 0, 8, 2.0))
    cluster_weight = gaussian(streams_of[4], (D, 3), D ** -0.5, 0.09375)
    proj_one = gaussian(streams_of[5], (D, P1), D ** -0.5, 0.09375, ((0, 8),))
    proj_two = gaussian(streams_of[6], (D, P2), D ** -0.5, 0.09375, ((0, 8),))
    proj_three = gaussian(streams_of[7], (D, P3), D ** -0.5, 0.09375, ((0, 8),))
    out_one = gaussian(streams_of[8], (P1, V1), P1 ** -0.5, 0.1875, ((1, 8),))
    out_two = gaussian(streams_of[9], (P2, V2), P2 ** -0.5, 0.375, ((1, 8),))
    out_three = gaussian(streams_of[10], (P3, V3), P3 ** -0.5, 0.75, ((1, 8),))
    return {"hidden": hidden, "labels": labels, "targets": targets, "head_weight": head_weight, "cluster_weight": cluster_weight, "proj_one": proj_one, "proj_two": proj_two, "proj_three": proj_three, "out_one": out_one, "out_two": out_two, "out_three": out_three}


capping = 30.0

def capped(values):
    return capping * jnp.tanh(values / capping)

def cluster_slots(labels, cluster, capacity):
    member = labels == cluster
    placed = jnp.cumsum(member.astype(jnp.int32)) - 1
    slot_of = jnp.where(member, placed, capacity).astype(jnp.int32)
    order = jnp.arange(labels.shape[0], dtype=jnp.int32)
    slot_rows = jnp.zeros((capacity + 1,), jnp.int32).at[slot_of].set(order)[:capacity]
    filled = (jnp.arange(capacity, dtype=jnp.int32) < jnp.sum(member.astype(jnp.int32))).astype(jnp.float32)
    return (slot_rows, filled)

def reference(hidden, labels, targets, head_weight, cluster_weight, proj_one, proj_two, proj_three, out_one, out_two, out_three):
    groups = TOKENS // GRP_TOK
    capacity = GRP_TOK // 4
    factor = jnp.sqrt(jnp.float32(D))
    tails = ((proj_one, out_one), (proj_two, out_two), (proj_three, out_three))
    counts = jnp.stack([jnp.sum((labels == cluster).astype(jnp.float32)) for cluster in (1, 2, 3)])
    weights = TOKENS / (4.0 * counts)

    def group_terms(packed):
        rows, labs, aims = packed
        head_cap = capped(jnp.dot(rows, head_weight, preferred_element_type=jnp.float32))
        clus_cap = capped(jnp.dot(rows, cluster_weight, preferred_element_type=jnp.float32))
        head_exp = jnp.exp(head_cap)
        clus_exp = jnp.exp(clus_cap)
        total = lax.optimization_barrier(jnp.sum(head_exp, 1)) + lax.optimization_barrier(jnp.sum(clus_exp, 1))
        head_hit = ((labs == 0)[:, None] & (jnp.arange(HEAD, dtype=jnp.int32)[None, :] == aims[:, None])).astype(jnp.float32)
        clus_hit = (jnp.arange(3, dtype=jnp.int32)[None, :] + 1 == labs[:, None]).astype(jnp.float32)
        picked = lax.optimization_barrier(jnp.sum(head_hit * head_cap, 1)) + lax.optimization_barrier(jnp.sum(clus_hit * clus_cap, 1))
        token_loss = jnp.log(total) - picked
        head_grad = (factor * (head_exp / total[:, None] - head_hit) * (1.0 - (head_cap / capping) ** 2)).astype(jnp.bfloat16)
        clus_grad = factor * (clus_exp / total[:, None] - clus_hit) * (1.0 - (clus_cap / capping) ** 2)
        grads = jnp.dot(head_grad, head_weight.T, preferred_element_type=jnp.float32)
        grads = grads + jnp.dot(clus_grad, cluster_weight.astype(jnp.float32).T, precision=lax.Precision.HIGHEST)
        for number in range(3):
            proj, out = tails[number]
            slot_rows, filled = cluster_slots(labs, number + 1, capacity)
            latent = jnp.dot(rows[slot_rows], proj, preferred_element_type=jnp.float32)
            tail_cap = capped(jnp.dot(latent, out.astype(jnp.float32), precision=lax.Precision.HIGHEST))
            tail_exp = jnp.exp(tail_cap)
            tail_total = lax.optimization_barrier(jnp.sum(tail_exp, 1))
            tail_hit = (jnp.arange(out.shape[1], dtype=jnp.int32)[None, :] == aims[slot_rows][:, None]).astype(jnp.float32) * filled[:, None]
            tail_loss = (jnp.log(tail_total) - lax.optimization_barrier(jnp.sum(tail_hit * tail_cap, 1))) * filled
            tail_grad = (factor * (tail_exp / tail_total[:, None] - tail_hit) * (1.0 - (tail_cap / capping) ** 2) * filled[:, None]).astype(jnp.bfloat16)
            latent_grad = jnp.dot(tail_grad, out.T, preferred_element_type=jnp.float32)
            back = jnp.dot(latent_grad, proj.astype(jnp.float32).T, precision=lax.Precision.HIGHEST)
            token_loss = token_loss.at[slot_rows].add(weights[number] * tail_loss)
            grads = grads.at[slot_rows].add(weights[number] * back)
        return (token_loss, grads)
    losses, grads = lax.map(group_terms, (hidden.reshape(groups, GRP_TOK, D), labels.reshape(groups, GRP_TOK), targets.reshape(groups, GRP_TOK)))
    token_loss = losses.reshape(TOKENS)
    mean_loss = jnp.sum(token_loss) / TOKENS
    return (token_loss, mean_loss, grads.reshape(TOKENS, D))
```

```python
import functools

import jax
import jax.numpy as jnp
from jax import lax
from jax.experimental import pallas as pl
from jax.experimental.pallas import tpu as pltpu
from jax.sharding import PartitionSpec as P


capping = 30.0
RING_LIMIT = 16


def capped(values):
    return capping * jnp.tanh(values * (1.0 / capping))


def butterfly_sum(values, axis, n):
    step = 1
    while step < n:
        pairs = [(i, i ^ step) for i in range(n)]
        other = lax.ppermute(values, axis, pairs)
        values = values + other
        step *= 2
    return values


def halving_sum(values, axis, n, steps):
    me = lax.axis_index(axis)
    bits = []
    for step in steps:
        bit = (me // step) % 2
        pairs = [(i, i ^ step) for i in range(n)]
        half = values.shape[0] // 2
        send = lax.dynamic_slice_in_dim(values, (1 - bit) * half, half, 0)
        keep = lax.dynamic_slice_in_dim(values, bit * half, half, 0)
        values = keep + lax.ppermute(send, axis, pairs)
        bits.append((bit, pairs))
    for bit, pairs in reversed(bits):
        other = lax.ppermute(values, axis, pairs)
        first = bit == 0
        values = jnp.concatenate(
            [jnp.where(first, values, other), jnp.where(first, other, values)], 0
        )
    return values


def dot_nt(a, b):
    return lax.dot_general(a, b, (((1,), (1,)), ((), ())), preferred_element_type=jnp.float32)


def block_width(words, most):
    width = most
    while words % width:
        width -= 128
    return width


def column_of(row):
    return jnp.transpose(jnp.broadcast_to(row, (128, row.shape[1])))[:, 0:1]


def ring_kernel(
    n,
    factor,
    grad,
    aims,
    hi_one,
    hi_two,
    hi_three,
    lo_one,
    lo_two,
    lo_three,
    weight,
    out_one,
    out_two,
    out_three,
    head_back,
    gathered,
    stats,
    blocks,
    ring,
    term,
    buf_one,
    buf_two,
    buf_three,
    mix_one,
    mix_two,
    mix_three,
    acc_one,
    acc_two,
    acc_three,
    sum_acc,
    pick_acc,
    stat_all,
    summed,
    half_in,
    chunk_in,
    collected,
    block_sem,
    buf_sem,
    ring_send,
    ring_recv,
    stat_send,
    stat_recv,
    half_send,
    half_recv,
    chunk_send,
    chunk_recv,
):
    f32, bf16 = jnp.float32, jnp.bfloat16
    me = lax.axis_index("vocab")
    half_n = n // 2
    odd = me % 2
    line = me // 2
    spot = (1 - odd) * line + odd * (n - 1 - line)

    def at(place):
        place = place % n
        back = place // half_n
        return (1 - back) * (2 * place) + back * (2 * (n - 1 - place) + 1)

    neighbour = (at(spot + 1), at(spot + n - 1))
    barrier = pltpu.get_barrier_semaphore()
    for step in range(1, n):
        pl.semaphore_signal(
            barrier,
            inc=1,
            device_id={"vocab": (me + step) % n},
            device_id_type=pl.DeviceIdType.MESH,
        )

    width = blocks.shape[2]

    def block_copy(way, hop):
        place = at(spot + (n - 1 - hop if way == 0 else 1 + hop))
        start = pl.multiple_of(place * width, width)
        slot = hop % 2
        return pltpu.make_async_copy(
            weight.at[pl.ds(start, width), :], blocks.at[way, slot], block_sem.at[way, slot]
        )

    for hop in range(2):
        for way in range(2):
            block_copy(way, hop).start()

    kinds = []
    for number, (hi, lo, out, buf, mix, acc) in enumerate(
        (
            (hi_one, lo_one, out_one, buf_one, mix_one, acc_one),
            (hi_two, lo_two, out_two, buf_two, mix_two, acc_two),
            (hi_three, lo_three, out_three, buf_three, mix_three, acc_three),
        )
    ):
        words = out.shape[1]
        wide = buf.shape[2]
        kinds.append((number, hi, lo, out, buf, mix, acc, words, wide, words // wide))

    def fetch(kind, i, slot):
        number, _, _, out, buf, _, _, _, wide, _ = kind
        start = pl.multiple_of(i * wide, wide)
        return pltpu.make_async_copy(
            out.at[:, pl.ds(start, wide)], buf.at[slot], buf_sem.at[number, slot]
        )

    for kind in kinds:
        fetch(kind, 0, 0).start()
        number, acc = kind[0], kind[6]
        acc[...] = jnp.zeros_like(acc)
    sum_acc[...] = jnp.zeros_like(sum_acc)
    pick_acc[...] = jnp.zeros_like(pick_acc)
    capacity = hi_one.shape[0]

    def tail_steps(kind, first, last):
        number, hi, lo, out, buf, mix, acc, words, wide, count = kind
        rows = pl.ds(number * capacity, capacity)

        def body(i, carry):
            slot = i % 2
            fetch(kind, i, slot).wait()

            @pl.when(i + 1 < count)
            def _():
                fetch(kind, i + 1, 1 - slot).start()

            words_here = buf[slot]
            values = jnp.dot(hi[...], words_here, preferred_element_type=f32)
            values = values + jnp.dot(lo[...], words_here, preferred_element_type=f32)
            aim = aims[rows, :] - me * words - i * wide
            total = sum_acc[rows, :]
            pick = pick_acc[rows, :]
            lane = lax.broadcasted_iota(jnp.int32, (capacity, 128), 1)
            for j in range(0, wide, 128):
                ratio = jnp.tanh(values[:, j : j + 128] * (1.0 / capping))
                cap = capping * ratio
                power = jnp.exp(cap)
                hit = lane + j == aim
                total = total + power
                pick = pick + jnp.where(hit, cap, 0.0)
                slope = 1.0 - ratio * ratio
                mix[0:capacity, j : j + 128] = jnp.where(hit, 0.0, power * slope).astype(bf16)
                mix[capacity : 2 * capacity, j : j + 128] = jnp.where(hit, 1.0, 0.0).astype(bf16)
            sum_acc[rows, :] = total
            pick_acc[rows, :] = pick
            acc[...] += dot_nt(mix[...], words_here)
            return carry

        lax.fori_loop(first, last, body, 0)

    capacity_all = 3 * capacity

    def stat_copy(step, index):
        return pltpu.make_async_remote_copy(
            src_ref=stat_all.at[index],
            dst_ref=stat_all.at[index],
            send_sem=stat_send.at[step - 1],
            recv_sem=stat_recv.at[step - 1],
            device_id={"vocab": (me + step) % n},
            device_id_type=pl.DeviceIdType.MESH,
        )

    def share_stats():
        own = jnp.zeros((8, capacity_all), f32)
        sums = jnp.sum(jnp.transpose(sum_acc[...]), axis=0, keepdims=True)
        picks = jnp.sum(jnp.transpose(pick_acc[...]), axis=0, keepdims=True)
        line_of = lax.broadcasted_iota(jnp.int32, (8, capacity_all), 0)
        own = jnp.where(line_of == 0, sums, jnp.where(line_of == 1, picks, 0.0))
        stat_all[me] = own
        for step in range(1, n):
            stat_copy(step, me).start()

    rows_half = capacity // 2
    lines = half_n
    rows_chunk = rows_half // lines
    own_half = pl.multiple_of(odd * rows_half, rows_half)
    other_half = pl.multiple_of((1 - odd) * rows_half, rows_half)
    partner = me + 1 - 2 * odd

    def half_copy(number, source, target):
        return pltpu.make_async_remote_copy(
            src_ref=source,
            dst_ref=target,
            send_sem=half_send.at[number],
            recv_sem=half_recv.at[number],
            device_id={"vocab": partner},
            device_id_type=pl.DeviceIdType.MESH,
        )

    first_half = half_copy(0, summed.at[pl.ds(other_half, rows_half), :], half_in)
    last_half = half_copy(
        1,
        collected.at[pl.ds(own_half, rows_half), :],
        collected.at[pl.ds(own_half, rows_half), :],
    )

    def chunk_rows(which):
        return pl.ds(pl.multiple_of(odd * rows_half + which * rows_chunk, rows_chunk), rows_chunk)

    def chunk_copy(phase, step):
        peer = (line + step) % lines
        if phase == 0:
            source, target = summed.at[chunk_rows(peer), :], chunk_in.at[step - 1]
        else:
            source = target = collected.at[chunk_rows(line), :]
        return pltpu.make_async_remote_copy(
            src_ref=source,
            dst_ref=target,
            send_sem=chunk_send.at[phase, step - 1],
            recv_sem=chunk_recv.at[phase, step - 1],
            device_id={"vocab": 2 * peer + odd},
            device_id_type=pl.DeviceIdType.MESH,
        )

    def finish_stats():
        for step in range(1, n):
            stat_copy(step, me).wait_recv()
        whole = stat_all[0]
        for index in range(1, n):
            whole = whole + stat_all[index]
        stats[...] = whole
        offset = 0
        for kind in kinds:
            number, acc, words = kind[0], kind[6], kind[7]
            rows = slice(number * capacity, (number + 1) * capacity)
            total = column_of(whole[0:1, rows])
            pick = jnp.sum(pick_acc[rows, :], axis=1, keepdims=True)
            aim = aims[rows, :]
            local = aim - me * words
            ratio = pick * (1.0 / capping)
            peak = (factor * (jnp.exp(pick) / total - 1.0) * (1.0 - ratio * ratio)).astype(bf16)
            here = jnp.logical_and(local >= 0, local < words)
            peak = jnp.where(here, peak.astype(f32), 0.0)
            scale = jnp.where(aim >= 0, factor / total, 0.0)
            size = acc.shape[1]
            summed[:, offset : offset + size] = (
                scale * acc[0:capacity, :] + peak * acc[capacity : 2 * capacity, :]
            )
            offset += size
        first_half.start()

    def spread_chunks():
        first_half.wait_recv()
        rows = pl.ds(own_half, rows_half)
        summed[rows, :] = summed[rows, :] + half_in[...]
        for step in range(1, lines):
            chunk_copy(0, step).start()

    def gather_chunks():
        rows = chunk_rows(line)
        whole = summed[rows, :]
        for step in range(1, lines):
            chunk_copy(0, step).wait_recv()
            whole = whole + chunk_in[step - 1]
        collected[rows, :] = whole
        for step in range(1, lines):
            chunk_copy(1, step).start()

    def swap_halves():
        for step in range(1, lines):
            chunk_copy(1, step).wait_recv()
        last_half.start()

    def take_result():
        last_half.wait_recv()
        gathered[...] = collected[...]

    rows_way = grad.shape[0] // 2
    rows_part = rows_way // 2

    def product(way, hop):
        block_copy(way, hop).wait()
        part = grad[way * rows_way : (way + 1) * rows_way, :]
        return dot_nt(part, blocks[way, hop % 2])

    def next_block(way, hop):
        if hop + 2 < n:
            block_copy(way, hop + 2).start()

    def hop_copy(way, part, hop):
        rows = pl.ds(part * rows_part, rows_part)
        return pltpu.make_async_remote_copy(
            src_ref=ring.at[way, hop, rows, :],
            dst_ref=ring.at[way, hop + 1, rows, :],
            send_sem=ring_send.at[way, part, hop],
            recv_sem=ring_recv.at[way, part, hop],
            device_id={"vocab": neighbour[way]},
            device_id_type=pl.DeviceIdType.MESH,
        )

    one, two, three = kinds

    def pieces(kind, times):
        count = kind[9]
        edges = [count * i // times for i in range(times + 1)]
        return [
            functools.partial(tail_steps, kind, edges[i], edges[i + 1]) for i in range(times)
        ]

    slots = pieces(one, 2) + pieces(two, 2) + pieces(three, 3)
    slots += [share_stats, finish_stats, spread_chunks, gather_chunks, swap_halves]
    work = [[] for _ in range(2 * (n - 1))]
    for i, piece in enumerate(slots):
        work[i * len(work) // (len(slots) + 1)].append(piece)
    work[-1].append(take_result)

    pl.semaphore_wait(barrier, n - 1)
    for way in range(2):
        ring[way, 0] = product(way, 0)
        next_block(way, 0)
        for part in range(2):
            hop_copy(way, part, 0).start()
    for way in range(2):
        term[way] = product(way, 1)
        next_block(way, 1)
    for hop in range(n - 1):
        for part in range(2):
            rows = pl.ds(part * rows_part, rows_part)
            for way in range(2):
                hop_copy(way, part, hop).wait_recv()
                held = ring[way, hop + 1, rows, :] + term[way, rows, :]
                if hop < n - 2:
                    ring[way, hop + 1, rows, :] = held
                    hop_copy(way, part, hop + 1).start()
                else:
                    head_back[pl.ds(way * rows_way + part * rows_part, rows_part), :] = held
            if part == 1 and hop < n - 2:
                for way in range(2):
                    term[way] = product(way, hop + 2)
                    next_block(way, hop + 2)
            for piece in work[2 * hop + part]:
                piece()
    for way in range(2):
        for part in range(2):
            for hop in range(n - 1):
                hop_copy(way, part, hop).wait_send()
    for step in range(1, n):
        stat_copy(step, me).wait_send()
    first_half.wait_send()
    last_half.wait_send()
    for phase in range(2):
        for step in range(1, lines):
            chunk_copy(phase, step).wait_send()


def ring_and_tails(n, factor, grad, aims, highs, lows, weight, outs, width):
    f32, bf16 = jnp.float32, jnp.bfloat16
    tokens = grad.shape[0]
    capacity = highs[0].shape[0]
    sizes = [out.shape[0] for out in outs]
    wides = [
        block_width(out.shape[1], most) for out, most in zip(outs, (1024, 2048, 2048))
    ]
    lines = n // 2
    vmem = pl.BlockSpec(memory_space=pltpu.VMEM)
    hbm = pl.BlockSpec(memory_space=pl.ANY)
    dma = pltpu.SemaphoreType.DMA
    return pl.pallas_call(
        functools.partial(ring_kernel, n, factor),
        out_shape=(
            jax.ShapeDtypeStruct((tokens, width), f32),
            jax.ShapeDtypeStruct((capacity, sum(sizes)), f32),
            jax.ShapeDtypeStruct((8, 3 * capacity), f32),
        ),
        in_specs=[vmem] * 8 + [hbm] * 4,
        out_specs=(vmem, vmem, vmem),
        scratch_shapes=[
            pltpu.VMEM((2, 2, width, weight.shape[1]), bf16),
            pltpu.VMEM((2, n, tokens // 2, width), f32),
            pltpu.VMEM((2, tokens // 2, width), f32),
        ]
        + [pltpu.VMEM((2, size, wide), bf16) for size, wide in zip(sizes, wides)]
        + [pltpu.VMEM((2 * capacity, wide), bf16) for wide in wides]
        + [pltpu.VMEM((2 * capacity, size), f32) for size in sizes]
        + [
            pltpu.VMEM((3 * capacity, 128), f32),
            pltpu.VMEM((3 * capacity, 128), f32),
            pltpu.VMEM((n, 8, 3 * capacity), f32),
            pltpu.VMEM((capacity, sum(sizes)), f32),
            pltpu.VMEM((capacity // 2, sum(sizes)), f32),
            pltpu.VMEM((lines - 1, capacity // 2 // lines, sum(sizes)), f32),
            pltpu.VMEM((capacity, sum(sizes)), f32),
            dma((2, 2)),
            dma((3, 2)),
            dma((2, 2, n - 1)),
            dma((2, 2, n - 1)),
            dma((n - 1,)),
            dma((n - 1,)),
            dma((2,)),
            dma((2,)),
            dma((2, lines - 1)),
            dma((2, lines - 1)),
        ],
        compiler_params=pltpu.CompilerParams(
            collective_id=0, has_side_effects=True, vmem_limit_bytes=66_000_000
        ),
    )(grad, aims, *highs, *lows, weight, *outs)


def per_device(
    n,
    groups,
    hidden,
    labels,
    targets,
    head_weight,
    cluster_weight,
    proj_one,
    proj_two,
    proj_three,
    out_one,
    out_two,
    out_three,
):
    f32, bf16 = jnp.float32, jnp.bfloat16
    tokens = hidden.shape[0]
    width = proj_one.shape[0]
    head_local = head_weight.shape[1]
    capacity = tokens // 4
    all_tokens = tokens * groups
    vocab_index = lax.axis_index("vocab")
    feat_start = vocab_index * width
    factor = jnp.sqrt(f32(hidden.shape[1]))
    projs = (proj_one, proj_two, proj_three)
    outs = (out_one, out_two, out_three)

    member = labels[None, :] == jnp.arange(1, 4, dtype=jnp.int32)[:, None]
    local_counts = jnp.sum(member.astype(f32), 1)
    row = jnp.arange(tokens, dtype=jnp.int32)
    upto = (row[:, None] <= row[None, :]).astype(bf16)
    placed = jnp.dot(member.astype(bf16), upto, preferred_element_type=f32).astype(jnp.int32) - 1
    offsets = jnp.arange(3, dtype=jnp.int32)[:, None] * capacity
    slot_of = jnp.sum(jnp.where(member, placed + offsets + 1, 0), 0) - 1
    slot_ids = jnp.arange(3 * capacity, dtype=jnp.int32)
    chosen = slot_ids[:, None] == slot_of[None, :]
    select = chosen.astype(bf16)
    slot_aims = jnp.sum(jnp.where(chosen, targets[None, :] + 1, 0), 1) - 1
    filled = (slot_aims >= 0).astype(f32)

    own_features = lax.dynamic_slice_in_dim(hidden, feat_start, width, 1)
    picked_rows = jnp.dot(select, own_features, preferred_element_type=f32).astype(bf16)
    latent_parts = []
    for number in range(3):
        chunk = picked_rows[number * capacity : (number + 1) * capacity]
        latent_parts.append(jnp.dot(chunk, projs[number], preferred_element_type=f32))
    powers = []
    step = 1
    while step < n:
        powers.append(step)
        step *= 2
    turned = powers[1:] + powers[:1]
    joined = jnp.concatenate([latent_parts[1], latent_parts[2]], 1)
    joined = halving_sum(joined, "vocab", n, turned)
    width_two = projs[1].shape[1]
    latents = [
        halving_sum(latent_parts[0], "vocab", n, powers),
        joined[:, :width_two],
        joined[:, width_two:],
    ]
    counts = butterfly_sum(local_counts, "dp", groups)
    weights = all_tokens / (4.0 * counts)

    head_cap = capped(jnp.dot(hidden, head_weight, preferred_element_type=f32))
    head_sum = jnp.sum(jnp.exp(head_cap), 1)
    head_sum = butterfly_sum(head_sum, "vocab", n)
    clus_cap = capped(jnp.dot(hidden, cluster_weight, preferred_element_type=f32))
    clus_exp = jnp.exp(clus_cap)
    clus_hit = (jnp.arange(3, dtype=jnp.int32)[None, :] + 1 == labels[:, None]).astype(f32)
    head_aims = jnp.where(labels == 0, targets, -1) - vocab_index * head_local
    head_hit = jnp.arange(head_local, dtype=jnp.int32)[None, :] == head_aims[:, None]
    total = head_sum + jnp.sum(clus_exp, 1)
    scale = factor / total
    kept_cap = lax.optimization_barrier(head_cap)
    head_pick = jnp.sum(jnp.where(head_hit, kept_cap, 0.0), 1)
    slope = 1.0 - (kept_cap * (1.0 / capping)) ** 2
    head_grad = (
        (jnp.exp(kept_cap) * scale[:, None] - jnp.where(head_hit, factor, 0.0)) * slope
    ).astype(bf16)
    clus_grad = (clus_exp * scale[:, None] - factor * clus_hit) * (
        1.0 - (clus_cap * (1.0 / capping)) ** 2
    )
    if n <= RING_LIMIT:
        highs, lows = [], []
        for latent in latents:
            high = lax.reduce_precision(latent, 8, 7)
            highs.append(high.astype(bf16))
            lows.append((latent - high).astype(bf16))
        head_back, latent_grad, stats = ring_and_tails(
            n,
            float(hidden.shape[1]) ** 0.5,
            head_grad,
            slot_aims[:, None],
            highs,
            lows,
            head_weight,
            outs,
            width,
        )
        width_one = projs[0].shape[1]
        latent_grads = [
            latent_grad[:, :width_one],
            latent_grad[:, width_one : width_one + width_two],
            latent_grad[:, width_one + width_two :],
        ]
        tail_totals, tail_picks = stats[0], stats[1]
    else:
        head_terms = jnp.einsum("tv,fv->tf", head_grad, head_weight, preferred_element_type=f32)
        head_back = lax.psum_scatter(head_terms, "vocab", scatter_dimension=1, tiled=True)

        tail_caps, tail_hits, tail_sums, tail_picks = [None] * 3, [None] * 3, [None] * 3, [None] * 3
        for number in (1, 2, 0):
            out = outs[number]
            tail_cap = capped(
                jnp.dot(latents[number], out.astype(f32), precision=lax.Precision.HIGH)
            )
            aims = slot_aims[number * capacity : (number + 1) * capacity]
            aims = jnp.where(aims >= 0, aims, -1) - vocab_index * out.shape[1]
            aims = jnp.where(slot_aims[number * capacity : (number + 1) * capacity] >= 0, aims, -1)
            tail_hits[number] = jnp.arange(out.shape[1], dtype=jnp.int32)[None, :] == aims[:, None]
            tail_sums[number] = jnp.sum(jnp.exp(tail_cap), 1)
            tail_caps[number] = lax.optimization_barrier(tail_cap)
            tail_picks[number] = jnp.sum(jnp.where(tail_hits[number], tail_caps[number], 0.0), 1)
        tail_totals = butterfly_sum(jnp.concatenate(tail_sums), "vocab", n)
        tail_scales = factor * filled / tail_totals
        grad_parts = [None] * 3
        for number in (0, 1, 2):
            cap = tail_caps[number]
            tail_scale = tail_scales[number * capacity : (number + 1) * capacity]
            tail_grad = (
                (jnp.exp(cap) * tail_scale[:, None] - jnp.where(tail_hits[number], factor, 0.0))
                * (1.0 - (cap * (1.0 / capping)) ** 2)
            ).astype(bf16)
            grad_parts[number] = jnp.einsum(
                "sv,pv->sp", tail_grad, outs[number], preferred_element_type=f32
            )
        grad_one = halving_sum(grad_parts[0], "vocab", n, powers)
        grad_rest = halving_sum(jnp.concatenate([grad_parts[1], grad_parts[2]], 1), "vocab", n, turned)
        latent_grads = [grad_one, grad_rest[:, :width_two], grad_rest[:, width_two:]]
        tail_picks = butterfly_sum(jnp.concatenate(tail_picks), "vocab", n)

    backs = []
    for number in range(3):
        back = jnp.einsum(
            "sp,fp->sf",
            latent_grads[number],
            projs[number].astype(f32),
            precision=lax.Precision.HIGH,
        )
        backs.append(weights[number] * back)
    back = jnp.concatenate(backs, 0)
    back_top = lax.reduce_precision(back, 8, 7)
    back_rest = (back - back_top).astype(bf16)
    back_top = back_top.astype(bf16)
    pick_slots = functools.partial(jnp.einsum, "st,sf->tf", preferred_element_type=f32)
    tail_back = pick_slots(select, back_top) + pick_slots(select, back_rest)
    clus_rows = lax.dynamic_slice_in_dim(cluster_weight, feat_start, width, 0).astype(f32)
    clus_back = (
        clus_grad[:, 0:1] * clus_rows[:, 0][None, :]
        + clus_grad[:, 1:2] * clus_rows[:, 1][None, :]
        + clus_grad[:, 2:3] * clus_rows[:, 2][None, :]
    )
    grads = head_back + (tail_back + clus_back)

    head_pick = butterfly_sum(head_pick, "vocab", n)
    head_loss = jnp.log(total) - head_pick - jnp.sum(clus_hit * clus_cap, 1)
    tail_loss = (jnp.log(tail_totals) - tail_picks) * filled
    slot_weights = jnp.repeat(weights, capacity)
    tail_loss = tail_loss * slot_weights
    token_loss = head_loss + jnp.sum(jnp.where(chosen, tail_loss[:, None], 0.0), 0)
    loss_sum = butterfly_sum(jnp.sum(token_loss)[None], "dp", groups)
    mean_loss = loss_sum[0] / all_tokens
    return (token_loss, mean_loss, grads)


def solution(mesh):
    body = functools.partial(per_device, mesh.shape["vocab"], mesh.shape["dp"])
    return jax.shard_map(
        body,
        mesh=mesh,
        in_specs=(
            P("dp", None),
            P("dp"),
            P("dp"),
            P(None, "vocab"),
            P(),
            P("vocab", None),
            P("vocab", None),
            P("vocab", None),
            P(None, "vocab"),
            P(None, "vocab"),
            P(None, "vocab"),
        ),
        out_specs=(P("dp"), P(), P("dp", "vocab")),
        check_vma=False,
    )
```

```python
import functools

import jax
import jax.numpy as jnp
from jax import lax
from jax.experimental import pallas as pl
from jax.experimental.pallas import tpu as pltpu
from jax.sharding import PartitionSpec as P


capping = 30.0
RING_LIMIT = 16


def capped(values):
    return capping * jnp.tanh(values * (1.0 / capping))


def butterfly_sum(values, axis, n):
    step = 1
    while step < n:
        pairs = [(i, i ^ step) for i in range(n)]
        other = lax.ppermute(values, axis, pairs)
        values = values + other
        step *= 2
    return values


def halving_sum(values, axis, n, steps):
    me = lax.axis_index(axis)
    bits = []
    for step in steps:
        bit = (me // step) % 2
        pairs = [(i, i ^ step) for i in range(n)]
        half = values.shape[0] // 2
        send = lax.dynamic_slice_in_dim(values, (1 - bit) * half, half, 0)
        keep = lax.dynamic_slice_in_dim(values, bit * half, half, 0)
        values = keep + lax.ppermute(send, axis, pairs)
        bits.append((bit, pairs))
    for bit, pairs in reversed(bits):
        other = lax.ppermute(values, axis, pairs)
        first = bit == 0
        values = jnp.concatenate(
            [jnp.where(first, values, other), jnp.where(first, other, values)], 0
        )
    return values


def dot_nt(a, b):
    return lax.dot_general(a, b, (((1,), (1,)), ((), ())), preferred_element_type=jnp.float32)


def block_width(words, most):
    width = most
    while words % width:
        width -= 128
    return width


def column_of(row):
    return jnp.transpose(jnp.broadcast_to(row, (128, row.shape[1])))[:, 0:1]


def peer_copy(source, target, send_sem, recv_sem, index):
    return pltpu.make_async_remote_copy(
        src_ref=source,
        dst_ref=target,
        send_sem=send_sem,
        recv_sem=recv_sem,
        device_id={"vocab": index},
        device_id_type=pl.DeviceIdType.MESH,
    )


def greet(n, me):
    barrier = pltpu.get_barrier_semaphore()
    for step in range(1, n):
        pl.semaphore_signal(
            barrier,
            inc=1,
            device_id={"vocab": (me + step) % n},
            device_id_type=pl.DeviceIdType.MESH,
        )
    return barrier


def group_of(n, me, rows_half):
    odd = me % 2
    line = me // 2
    rows_chunk = rows_half // (n // 2)
    own_half = pl.ds(pl.multiple_of(odd * rows_half, rows_half), rows_half)
    other_half = pl.ds(pl.multiple_of((1 - odd) * rows_half, rows_half), rows_half)

    def chunk(which):
        return pl.ds(pl.multiple_of(odd * rows_half + which * rows_chunk, rows_chunk), rows_chunk)

    return odd, line, me + 1 - 2 * odd, own_half, other_half, chunk


def scatter_phases(n, me, parts, refs):
    summed, half_in, chunk_in, half_send, half_recv, chunk_send, chunk_recv = refs
    lines = n // 2
    odd, line, partner, own_half, other_half, chunk = group_of(n, me, half_in.shape[0])

    def half_copy():
        return peer_copy(
            parts.at[other_half, :], half_in, half_send.at[0], half_recv.at[0], partner
        )

    def chunk_copy(step):
        peer = (line + step) % lines
        return peer_copy(
            summed.at[chunk(peer), :],
            chunk_in.at[step - 1],
            chunk_send.at[step - 1],
            chunk_recv.at[step - 1],
            2 * peer + odd,
        )

    def send_half():
        half_copy().start()

    def spread_chunks():
        half_copy().wait_recv()
        summed[own_half, :] = parts[own_half, :] + half_in[...]
        for step in range(1, lines):
            chunk_copy(step).start()

    def sum_chunks():
        whole = summed[chunk(line), :]
        for step in range(1, lines):
            chunk_copy(step).wait_recv()
            whole = whole + chunk_in[step - 1]
        return whole

    def drain():
        half_copy().wait_send()
        for step in range(1, lines):
            chunk_copy(step).wait_send()

    return send_half, spread_chunks, sum_chunks, drain


def gather_phases(n, me, refs):
    collected, half_send, half_recv, chunk_send, chunk_recv = refs
    lines = n // 2
    odd, line, partner, own_half, _, chunk = group_of(n, me, collected.shape[0] // 2)

    def half_copy():
        place = collected.at[own_half, :]
        return peer_copy(place, place, half_send.at[0], half_recv.at[0], partner)

    def chunk_copy(step):
        place = collected.at[chunk(line), :]
        return peer_copy(
            place,
            place,
            chunk_send.at[step - 1],
            chunk_recv.at[step - 1],
            2 * ((line + step) % lines) + odd,
        )

    def send_chunks(value):
        collected[chunk(line), :] = value
        for step in range(1, lines):
            chunk_copy(step).start()

    def swap_halves():
        for step in range(1, lines):
            chunk_copy(step).wait_recv()
        half_copy().start()

    def take_halves():
        half_copy().wait_recv()

    def drain():
        half_copy().wait_send()
        for step in range(1, lines):
            chunk_copy(step).wait_send()

    return send_chunks, swap_halves, take_halves, drain


def scatter_scratch(n, capacity, size):
    lines = n // 2
    dma = pltpu.SemaphoreType.DMA
    return [
        pltpu.VMEM((capacity, size), jnp.float32),
        pltpu.VMEM((capacity // 2, size), jnp.float32),
        pltpu.VMEM((lines - 1, capacity // 2 // lines, size), jnp.float32),
        dma((1,)),
        dma((1,)),
        dma((lines - 1,)),
        dma((lines - 1,)),
    ]


def gather_scratch(n, capacity, size):
    lines = n // 2
    dma = pltpu.SemaphoreType.DMA
    return [
        pltpu.VMEM((capacity, size), jnp.float32),
        dma((1,)),
        dma((1,)),
        dma((lines - 1,)),
        dma((lines - 1,)),
    ]


def split_pair(value):
    top = value.astype(jnp.bfloat16)
    return top, (value - top.astype(jnp.float32)).astype(jnp.bfloat16)


def spread_row(row):
    wide = jnp.broadcast_to(row.astype(jnp.float32), (128, row.shape[1]))
    return jnp.transpose(wide).astype(jnp.int32)


def share_row(n, me, stat_all, stat_send, stat_recv):
    def copy(step):
        return peer_copy(
            stat_all.at[me],
            stat_all.at[me],
            stat_send.at[step - 1],
            stat_recv.at[step - 1],
            (me + step) % n,
        )

    def send(sums, picks):
        sums = jnp.sum(jnp.transpose(sums), axis=0, keepdims=True)
        picks = jnp.sum(jnp.transpose(picks), axis=0, keepdims=True)
        line_of = lax.broadcasted_iota(jnp.int32, stat_all.shape[1:], 0)
        stat_all[me] = jnp.where(line_of == 0, sums, jnp.where(line_of == 1, picks, 0.0))
        for step in range(1, n):
            copy(step).start()

    def take():
        for step in range(1, n):
            copy(step).wait_recv()
        whole = stat_all[0]
        for index in range(1, n):
            whole = whole + stat_all[index]
        return whole

    def drain():
        for step in range(1, n):
            copy(step).wait_send()

    return send, take, drain


def head_kernel(
    n,
    factor,
    hidden,
    table,
    cluster,
    proj_one,
    proj_two,
    proj_three,
    weight,
    grad,
    high,
    low,
    chunk_one,
    cluster_high,
    cluster_low,
    stats,
    columns,
    ratios,
    sum_acc,
    pick_acc,
    stat_all,
    aims,
    parts_one,
    parts_rest,
    select,
    column_sem,
    stat_send,
    stat_recv,
    *refs,
):
    f32, bf16 = jnp.float32, jnp.bfloat16
    me = lax.axis_index("vocab")
    barrier = greet(n, me)
    tokens = hidden.shape[0]
    wide = columns.shape[2]
    words = weight.shape[1]
    count = words // wide

    def fetch(i, slot):
        start = pl.multiple_of(i * wide, wide)
        return pltpu.make_async_copy(
            weight.at[:, pl.ds(start, wide)], columns.at[slot], column_sem.at[slot]
        )

    fetch(0, 0).start()
    capacity = tokens // 4
    width = proj_one.shape[0]
    slot_row = table[2:3, :]
    for base in range(0, 3 * capacity, capacity):
        slot = lax.broadcasted_iota(jnp.int32, (capacity, tokens), 0) + base
        select[base : base + capacity, :] = jnp.where(slot == slot_row, 1.0, 0.0).astype(bf16)
    own = pl.ds(pl.multiple_of(me * width, width), width)
    rows_all = jnp.dot(select[...], hidden[:, own], preferred_element_type=f32).astype(bf16)
    size_two = proj_two.shape[1]
    rest = parts_rest.shape[1]
    parts_one[...] = jnp.dot(rows_all[0:capacity], proj_one[...], preferred_element_type=f32)
    parts_rest[:, 0:size_two] = jnp.dot(
        rows_all[capacity : 2 * capacity], proj_two[...], preferred_element_type=f32
    )
    parts_rest[:, size_two:rest] = jnp.dot(
        rows_all[2 * capacity :], proj_three[...], preferred_element_type=f32
    )
    one_half, one_spread, one_sum, one_drain = scatter_phases(n, me, parts_one, refs[0:7])
    rest_half, rest_spread, rest_sum, rest_drain = scatter_phases(n, me, parts_rest, refs[7:14])
    rest_send, rest_swap, rest_take, rest_end = gather_phases(n, me, refs[14:19])
    send_stats, take_stats, drain_stats = share_row(n, me, stat_all, stat_send, stat_recv)
    pl.semaphore_wait(barrier, n - 1)
    rest_half()
    one_half()

    labels = spread_row(table[0:1, :])
    targets = spread_row(table[1:2, :])
    lanes = lax.broadcasted_iota(jnp.int32, (tokens, 128), 1)
    aims[...] = jnp.where(labels == 0, targets, -1) - me * words
    first = jnp.where(me == 0, 1.0, 0.0)
    ratio = jnp.tanh(
        jnp.dot(hidden[...], cluster[...], preferred_element_type=f32) * (1.0 / capping)
    )
    power = jnp.exp(capping * ratio)
    sum_acc[...] = first * jnp.where(lanes < 3, power, 0.0)
    pick_acc[...] = first * jnp.where(lanes + 1 == labels, capping * ratio, 0.0)

    turns = [
        rest_spread,
        lambda: rest_send(rest_sum()),
        one_spread,
        rest_swap,
    ]
    rows_part = tokens // 2

    def body(i, carry):
        slot = i % 2
        fetch(i, slot).wait()

        @pl.when(i + 1 < count)
        def _():
            fetch(i + 1, 1 - slot).start()

        for turn, phase in enumerate(turns):

            @pl.when(i == min(1 + turn * count // (len(turns) + 1), count - 1))
            def _(phase=phase):
                phase()

        here = pl.multiple_of(i * wide, wide)
        for part in range(2):
            rows = pl.ds(part * rows_part, rows_part)
            values = jnp.dot(hidden[rows, :], columns[slot], preferred_element_type=f32)
            ratio = jnp.tanh(values * (1.0 / capping))
            ratios[rows, pl.ds(here, wide)] = ratio
            cap = capping * ratio
            power = jnp.exp(cap)
            aim = aims[rows, :] - here
            lane = lax.broadcasted_iota(jnp.int32, (rows_part, 128), 1)
            total = sum_acc[rows, :]
            pick = pick_acc[rows, :]
            for j in range(0, wide, 128):
                total = total + power[:, j : j + 128]
                pick = pick + jnp.where(lane + j == aim, cap[:, j : j + 128], 0.0)
            sum_acc[rows, :] = total
            pick_acc[rows, :] = pick
        return carry

    lax.fori_loop(0, count, body, 0)
    send_stats(sum_acc[...], pick_acc[...])
    whole = take_stats()
    stats[...] = whole
    sum_acc[...] = factor / jnp.transpose(jnp.broadcast_to(whole[0:1, :], (128, tokens)))
    step_rows = 64

    def finish(r, carry):
        rows = pl.ds(pl.multiple_of(r * step_rows, step_rows), step_rows)
        scale = sum_acc[rows, :]
        aim = aims[rows, :]
        lane = lax.broadcasted_iota(jnp.int32, (step_rows, 128), 1)
        for j in range(0, ratios.shape[1], 128):
            ratio = ratios[rows, j : j + 128]
            share = jnp.exp(capping * ratio) * scale
            share = share - jnp.where(lane + j == aim, factor, 0.0)
            grad[rows, j : j + 128] = (share * (1.0 - ratio * ratio)).astype(bf16)
        return carry

    lax.fori_loop(0, tokens // step_rows, finish, 0)
    share = power * sum_acc[...] - jnp.where(lanes + 1 == labels, factor, 0.0)
    share = jnp.where(lanes < 3, share * (1.0 - ratio * ratio), 0.0)
    cluster_high[...], cluster_low[...] = split_pair(share)
    chunk_one[...] = one_sum()
    rest_take()
    high[...], low[...] = split_pair(refs[14][...])
    one_drain()
    rest_drain()
    rest_end()
    drain_stats()


def head_forward(n, factor, hidden, table, cluster, projs, weight):
    f32, bf16 = jnp.float32, jnp.bfloat16
    tokens, words = hidden.shape[0], weight.shape[1]
    capacity = tokens // 4
    size = projs[0].shape[1]
    rest = projs[1].shape[1] + projs[2].shape[1]
    wide = block_width(words, 256)
    vmem = pl.BlockSpec(memory_space=pltpu.VMEM)
    hbm = pl.BlockSpec(memory_space=pl.ANY)
    dma = pltpu.SemaphoreType.DMA
    return pl.pallas_call(
        functools.partial(head_kernel, n, factor),
        out_shape=(
            jax.ShapeDtypeStruct((tokens, words), bf16),
            jax.ShapeDtypeStruct((capacity, rest), bf16),
            jax.ShapeDtypeStruct((capacity, rest), bf16),
            jax.ShapeDtypeStruct((capacity // n, size), f32),
            jax.ShapeDtypeStruct((tokens, 128), bf16),
            jax.ShapeDtypeStruct((tokens, 128), bf16),
            jax.ShapeDtypeStruct((8, tokens), f32),
        ),
        in_specs=[vmem] * 6 + [hbm],
        out_specs=(vmem,) * 7,
        scratch_shapes=[
            pltpu.VMEM((2, weight.shape[0], wide), bf16),
            pltpu.VMEM((tokens, words), f32),
            pltpu.VMEM((tokens, 128), f32),
            pltpu.VMEM((tokens, 128), f32),
            pltpu.VMEM((n, 8, tokens), f32),
            pltpu.VMEM((tokens, 128), jnp.int32),
            pltpu.VMEM((capacity, size), f32),
            pltpu.VMEM((capacity, rest), f32),
            pltpu.VMEM((3 * capacity, tokens), bf16),
            dma((2,)),
            dma((n - 1,)),
            dma((n - 1,)),
        ]
        + scatter_scratch(n, capacity, size)
        + scatter_scratch(n, capacity, rest)
        + gather_scratch(n, capacity, rest),
        compiler_params=pltpu.CompilerParams(
            collective_id=1, has_side_effects=True, vmem_limit_bytes=60_000_000
        ),
    )(hidden, table, cluster, *projs, weight)


def ring_kernel(
    n,
    factor,
    grad,
    table,
    high,
    low,
    chunk_one,
    cluster_high,
    cluster_low,
    cluster_rows,
    proj_one,
    proj_two,
    proj_three,
    weights,
    weight,
    out_one,
    out_two,
    out_three,
    grads,
    stats,
    blocks,
    ring,
    term,
    buf_one,
    buf_two,
    buf_three,
    mix,
    acc_one,
    acc_two,
    acc_three,
    sum_acc,
    pick_acc,
    stat_one,
    stat_rest,
    given_one,
    given_rest,
    high_one,
    low_one,
    aims,
    joins,
    backs,
    block_sem,
    buf_sem,
    ring_send,
    ring_recv,
    stat_send,
    stat_recv,
    *refs,
):
    f32, bf16 = jnp.float32, jnp.bfloat16
    me = lax.axis_index("vocab")
    half_n = n // 2
    odd = me % 2
    line = me // 2
    spot = (1 - odd) * line + odd * (n - 1 - line)

    def at(place):
        place = place % n
        back = place // half_n
        return (1 - back) * (2 * place) + back * (2 * (n - 1 - place) + 1)

    neighbour = (at(spot + 1), at(spot + n - 1))
    barrier = greet(n, me)
    width = blocks.shape[2]

    def block_copy(way, hop):
        place = at(spot + (n - 1 - hop if way == 0 else 1 + hop))
        start = pl.multiple_of(place * width, width)
        slot = hop % 2
        return pltpu.make_async_copy(
            weight.at[pl.ds(start, width), :], blocks.at[way, slot], block_sem.at[way, slot]
        )

    for hop in range(2):
        for way in range(2):
            block_copy(way, hop).start()

    capacity = high.shape[0]
    tokens = grad.shape[0]
    kinds = []
    size_two = out_two.shape[0]
    for number, (out, buf, acc, proj, tops, rests, given, span) in enumerate(
        (
            (out_one, buf_one, acc_one, proj_one, high_one, low_one, given_one, slice(None)),
            (out_two, buf_two, acc_two, proj_two, high, low, given_rest, slice(0, size_two)),
            (
                out_three,
                buf_three,
                acc_three,
                proj_three,
                high,
                low,
                given_rest,
                slice(size_two, high.shape[1]),
            ),
        )
    ):
        words = out.shape[1]
        wide = buf.shape[2]
        kinds.append(
            (number, span, out, buf, acc, words, wide, words // wide, proj, tops, rests, given)
        )

    def fetch(kind, i, slot):
        number, out, buf, wide = kind[0], kind[2], kind[3], kind[6]
        start = pl.multiple_of(i * wide, wide)
        return pltpu.make_async_copy(
            out.at[:, pl.ds(start, wide)], buf.at[slot], buf_sem.at[number, slot]
        )

    for kind in kinds:
        fetch(kind, 0, 0).start()
        acc = kind[4]
        acc[...] = jnp.zeros_like(acc)
    sum_acc[...] = jnp.zeros_like(sum_acc)
    pick_acc[...] = jnp.zeros_like(pick_acc)

    def tail_steps(kind, first, last):
        number, span, out, buf, acc, words, wide, count, _, tops, rests, _ = kind
        rows = pl.ds(number * capacity, capacity)

        def body(i, carry):
            slot = i % 2
            fetch(kind, i, slot).wait()

            @pl.when(i + 1 < count)
            def _():
                fetch(kind, i + 1, 1 - slot).start()

            words_here = buf[slot]
            values = jnp.dot(tops[:, span], words_here, preferred_element_type=f32)
            values = values + jnp.dot(rests[:, span], words_here, preferred_element_type=f32)
            aim = aims[rows, :] - me * words - i * wide
            total = sum_acc[rows, :]
            pick = pick_acc[rows, :]
            lane = lax.broadcasted_iota(jnp.int32, (capacity, 128), 1)
            for j in range(0, wide, 128):
                ratio = jnp.tanh(values[:, j : j + 128] * (1.0 / capping))
                cap = capping * ratio
                power = jnp.exp(cap)
                hit = lane + j == aim
                total = total + power
                pick = pick + jnp.where(hit, cap, 0.0)
                slope = 1.0 - ratio * ratio
                mix[0:capacity, j : j + 128] = jnp.where(hit, 0.0, power * slope).astype(bf16)
                mix[capacity : 2 * capacity, j : j + 128] = jnp.where(hit, 1.0, 0.0).astype(bf16)
            sum_acc[rows, :] = total
            pick_acc[rows, :] = pick
            acc[...] += dot_nt(mix[:, 0:wide], words_here)
            return carry

        lax.fori_loop(first, last, body, 0)

    one_stats = share_row(n, me, stat_one, stat_send.at[0], stat_recv.at[0])
    rest_stats = share_row(n, me, stat_rest, stat_send.at[1], stat_recv.at[1])
    latent_send, latent_swap, latent_take, latent_end = gather_phases(n, me, refs[0:5])
    one_half, one_spread, one_sum, one_drain = scatter_phases(n, me, given_one, refs[5:12])
    one_send, one_swap, one_take, one_end = gather_phases(n, me, refs[12:17])
    rest_half, rest_spread, rest_sum, rest_drain = scatter_phases(n, me, given_rest, refs[17:24])
    rest_send, rest_swap, rest_take, rest_end = gather_phases(n, me, refs[24:29])
    one, two, three = kinds

    def set_up():
        slot_row = table[2:3, :]
        target_row = table[1:2, :].astype(f32)
        for base in range(0, 3 * capacity, 128):
            slot = lax.broadcasted_iota(jnp.int32, (128, tokens), 0) + base
            found = jnp.where(slot == slot_row, target_row + 1.0, 0.0)
            found = jnp.sum(found, axis=1, keepdims=True) - 1.0
            aims[base : base + 128, :] = jnp.broadcast_to(found, (128, 128)).astype(jnp.int32)
        slots_here = spread_row(slot_row)
        lanes = lax.broadcasted_iota(jnp.int32, (tokens, 128), 1)
        for base in range(0, 3 * capacity, 128):
            hit = lanes + base == slots_here
            joins[:, base : base + 128] = jnp.where(hit, 1.0, 0.0).astype(bf16)

    def take_latents():
        latent_take()
        high_one[...], low_one[...] = split_pair(refs[0][...])

    def share_stats(stats_of, first, last):
        rows = slice(first * capacity, last * capacity)
        stats_of[0](sum_acc[rows, :], pick_acc[rows, :])

    def finish_stats(stats_of, group, send_half):
        whole = stats_of[1]()
        first = group[0][0]
        stats[:, first * capacity : (first + len(group)) * capacity] = whole
        for number, span, _, _, acc, words, _, _, _, _, _, given in group:
            rows = slice(number * capacity, (number + 1) * capacity)
            here = slice((number - first) * capacity, (number - first + 1) * capacity)
            total = column_of(whole[0:1, here])
            pick = jnp.sum(pick_acc[rows, :], axis=1, keepdims=True)
            aim = aims[rows, 0:1]
            local = aim - me * words
            ratio = pick * (1.0 / capping)
            peak = (factor * (jnp.exp(pick) / total - 1.0) * (1.0 - ratio * ratio)).astype(bf16)
            inside = jnp.logical_and(local >= 0, local < words)
            peak = jnp.where(inside, peak.astype(f32), 0.0)
            scale = jnp.where(aim >= 0, factor / total, 0.0)
            given[:, span] = weights[number] * (
                scale * acc[0:capacity, :] + peak * acc[capacity : 2 * capacity, :]
            )
        send_half()

    def take_back(group, take, collected):
        take()
        for number, span, _, _, _, _, _, _, proj, _, _, _ in group:
            rows = slice(number * capacity, (number + 1) * capacity)
            top, lower = split_pair(collected[:, span])
            back = dot_nt(top, proj[...]) + dot_nt(lower, proj[...])
            backs[0, rows, :], backs[1, rows, :] = split_pair(back)

    def join_backs():
        total = jnp.dot(joins[...], backs[0], preferred_element_type=f32)
        total = total + jnp.dot(joins[...], backs[1], preferred_element_type=f32)
        total = total + jnp.dot(cluster_high[...], cluster_rows[...], preferred_element_type=f32)
        grads[...] = total + jnp.dot(
            cluster_low[...], cluster_rows[...], preferred_element_type=f32
        )

    rows_way = grad.shape[0] // 2
    rows_part = rows_way // 2

    def product(way, hop):
        block_copy(way, hop).wait()
        part = grad[way * rows_way : (way + 1) * rows_way, :]
        return dot_nt(part, blocks[way, hop % 2])

    def next_block(way, hop):
        if hop + 2 < n:
            block_copy(way, hop + 2).start()

    def hop_copy(way, part, hop):
        rows = pl.ds(part * rows_part, rows_part)
        return peer_copy(
            ring.at[way, hop, rows, :],
            ring.at[way, hop + 1, rows, :],
            ring_send.at[way, part, hop],
            ring_recv.at[way, part, hop],
            neighbour[way],
        )

    def pieces(kind, times):
        count = kind[7]
        edges = [count * i // times for i in range(times + 1)]
        return [
            functools.partial(tail_steps, kind, edges[i], edges[i + 1]) for i in range(times)
        ]

    three_a, three_b, three_c = pieces(three, 3)
    two_a, two_b = pieces(two, 2)
    one_a, one_b = pieces(one, 2)
    work_share = functools.partial
    plan = [
        [set_up, three_a],
        [latent_swap, three_b],
        [three_c],
        [take_latents, two_a],
        [two_b, work_share(share_stats, rest_stats, 1, 3)],
        [work_share(finish_stats, rest_stats, (two, three), rest_half), one_a],
        [rest_spread, one_b, work_share(share_stats, one_stats, 0, 1)],
        [
            work_share(finish_stats, one_stats, (one,), one_half),
            lambda: rest_send(rest_sum()),
        ],
        [one_spread, rest_swap],
        [lambda: one_send(one_sum()), work_share(take_back, (two, three), rest_take, refs[24])],
        [one_swap],
        [work_share(take_back, (one,), one_take, refs[12]), join_backs],
    ]
    work = [[] for _ in range(2 * (n - 1))]
    for i, group in enumerate(plan):
        work[i * (len(work) - 2) // len(plan)] += group

    pl.semaphore_wait(barrier, n - 1)
    for way in range(2):
        ring[way, 0] = product(way, 0)
        next_block(way, 0)
        for part in range(2):
            hop_copy(way, part, 0).start()
    latent_send(chunk_one[...])
    for way in range(2):
        term[way] = product(way, 1)
        next_block(way, 1)
    for hop in range(n - 1):
        for part in range(2):
            rows = pl.ds(part * rows_part, rows_part)
            for way in range(2):
                hop_copy(way, part, hop).wait_recv()
                held = ring[way, hop + 1, rows, :] + term[way, rows, :]
                if hop < n - 2:
                    ring[way, hop + 1, rows, :] = held
                    hop_copy(way, part, hop + 1).start()
                else:
                    grads[pl.ds(way * rows_way + part * rows_part, rows_part), :] += held
            if part == 1 and hop < n - 2:
                for way in range(2):
                    term[way] = product(way, hop + 2)
                    next_block(way, hop + 2)
            for piece in work[2 * hop + part]:
                piece()
    for way in range(2):
        for part in range(2):
            for hop in range(n - 1):
                hop_copy(way, part, hop).wait_send()
    one_stats[2]()
    rest_stats[2]()
    latent_end()
    one_drain()
    one_end()
    rest_drain()
    rest_end()


def ring_and_tails(n, factor, grad, table, latents, clusters, projs, weights, weight, outs):
    f32, bf16 = jnp.float32, jnp.bfloat16
    tokens = grad.shape[0]
    capacity = latents[0].shape[0]
    width = projs[0].shape[0]
    rest = latents[0].shape[1]
    sizes = [out.shape[0] for out in outs]
    wides = [block_width(out.shape[1], 1024) for out in outs]
    vmem = pl.BlockSpec(memory_space=pltpu.VMEM)
    smem = pl.BlockSpec(memory_space=pltpu.SMEM)
    hbm = pl.BlockSpec(memory_space=pl.ANY)
    dma = pltpu.SemaphoreType.DMA
    return pl.pallas_call(
        functools.partial(ring_kernel, n, factor),
        out_shape=(
            jax.ShapeDtypeStruct((tokens, width), f32),
            jax.ShapeDtypeStruct((8, 3 * capacity), f32),
        ),
        in_specs=[vmem] * 11 + [smem] + [hbm] * 4,
        out_specs=(vmem, vmem),
        scratch_shapes=[
            pltpu.VMEM((2, 2, width, weight.shape[1]), bf16),
            pltpu.VMEM((2, n, tokens // 2, width), f32),
            pltpu.VMEM((2, tokens // 2, width), f32),
        ]
        + [pltpu.VMEM((2, size, wide), bf16) for size, wide in zip(sizes, wides)]
        + [pltpu.VMEM((2 * capacity, max(wides)), bf16)]
        + [pltpu.VMEM((2 * capacity, size), f32) for size in sizes]
        + [
            pltpu.VMEM((3 * capacity, 128), f32),
            pltpu.VMEM((3 * capacity, 128), f32),
            pltpu.VMEM((n, 8, capacity), f32),
            pltpu.VMEM((n, 8, 2 * capacity), f32),
            pltpu.VMEM((capacity, sizes[0]), f32),
            pltpu.VMEM((capacity, rest), f32),
            pltpu.VMEM((capacity, sizes[0]), bf16),
            pltpu.VMEM((capacity, sizes[0]), bf16),
            pltpu.VMEM((3 * capacity, 128), jnp.int32),
            pltpu.VMEM((tokens, 3 * capacity), bf16),
            pltpu.VMEM((2, 3 * capacity, width), bf16),
            dma((2, 2)),
            dma((3, 2)),
            dma((2, 2, n - 1)),
            dma((2, 2, n - 1)),
            dma((2, n - 1)),
            dma((2, n - 1)),
        ]
        + gather_scratch(n, capacity, sizes[0])
        + scatter_scratch(n, capacity, sizes[0])
        + gather_scratch(n, capacity, sizes[0])
        + scatter_scratch(n, capacity, rest)
        + gather_scratch(n, capacity, rest),
        compiler_params=pltpu.CompilerParams(
            collective_id=0, has_side_effects=True, vmem_limit_bytes=66_000_000
        ),
    )(grad, table, *latents, *clusters, *projs, weights, weight, *outs)


def per_device(
    n,
    groups,
    hidden,
    labels,
    targets,
    head_weight,
    cluster_weight,
    proj_one,
    proj_two,
    proj_three,
    out_one,
    out_two,
    out_three,
):
    f32, bf16 = jnp.float32, jnp.bfloat16
    tokens = hidden.shape[0]
    width = proj_one.shape[0]
    head_local = head_weight.shape[1]
    capacity = tokens // 4
    all_tokens = tokens * groups
    vocab_index = lax.axis_index("vocab")
    feat_start = vocab_index * width
    factor = jnp.sqrt(f32(hidden.shape[1]))
    projs = (proj_one, proj_two, proj_three)
    outs = (out_one, out_two, out_three)

    member = labels[None, :] == jnp.arange(1, 4, dtype=jnp.int32)[:, None]
    local_counts = jnp.sum(member.astype(f32), 1)
    row = jnp.arange(tokens, dtype=jnp.int32)
    upto = (row[:, None] <= row[None, :]).astype(bf16)
    placed = jnp.dot(member.astype(bf16), upto, preferred_element_type=f32).astype(jnp.int32) - 1
    offsets = jnp.arange(3, dtype=jnp.int32)[:, None] * capacity
    slot_of = jnp.sum(jnp.where(member, placed + offsets + 1, 0), 0) - 1
    slot_ids = jnp.arange(3 * capacity, dtype=jnp.int32)
    chosen = slot_ids[:, None] == slot_of[None, :]
    select = chosen.astype(bf16)
    slot_aims = jnp.sum(jnp.where(chosen, targets[None, :] + 1, 0), 1) - 1
    filled = (slot_aims >= 0).astype(f32)

    own_features = lax.dynamic_slice_in_dim(hidden, feat_start, width, 1)
    picked_rows = jnp.dot(select, own_features, preferred_element_type=f32).astype(bf16)
    latent_parts = []
    for number in range(3):
        chunk = picked_rows[number * capacity : (number + 1) * capacity]
        latent_parts.append(jnp.dot(chunk, projs[number], preferred_element_type=f32))
    counts = butterfly_sum(local_counts, "dp", groups)
    weights = all_tokens / (4.0 * counts)
    clus_cap = capped(jnp.dot(hidden, cluster_weight, preferred_element_type=f32))
    clus_exp = jnp.exp(clus_cap)
    clus_hit = (jnp.arange(3, dtype=jnp.int32)[None, :] + 1 == labels[:, None]).astype(f32)
    clus_sum = jnp.sum(clus_exp, 1)
    clus_slope = 1.0 - (clus_cap * (1.0 / capping)) ** 2
    head_aims = jnp.where(labels == 0, targets, -1) - vocab_index * head_local
    clus_rows = lax.dynamic_slice_in_dim(cluster_weight, feat_start, width, 0)

    if n <= RING_LIMIT:
        scale_of = float(hidden.shape[1]) ** 0.5
        table = jnp.concatenate(
            [
                jnp.stack([labels, targets, slot_of]),
                jnp.zeros((5, tokens), jnp.int32),
            ],
            0,
        )
        padded = jnp.pad(cluster_weight, ((0, 0), (0, 125)))
        grad, high, low, chunk, clus_high, clus_low, head_stats = head_forward(
            n, scale_of, hidden, table, padded, projs, head_weight
        )
        clus_lines = jnp.pad(jnp.transpose(clus_rows), ((0, 125), (0, 0)))
        grads, stats = ring_and_tails(
            n,
            scale_of,
            grad,
            table,
            (high, low, chunk),
            (clus_high, clus_low, clus_lines),
            projs,
            weights,
            head_weight,
            outs,
        )
        head_loss = jnp.log(head_stats[0]) - head_stats[1]
        tail_totals, tail_picks = stats[0], stats[1]
    else:
        powers = []
        step = 1
        while step < n:
            powers.append(step)
            step *= 2
        turned = powers[1:] + powers[:1]
        joined = jnp.concatenate([latent_parts[1], latent_parts[2]], 1)
        joined = halving_sum(joined, "vocab", n, turned)
        width_two = projs[1].shape[1]
        latents = [
            halving_sum(latent_parts[0], "vocab", n, powers),
            joined[:, :width_two],
            joined[:, width_two:],
        ]
        head_cap = capped(jnp.dot(hidden, head_weight, preferred_element_type=f32))
        head_sum = jnp.sum(jnp.exp(head_cap), 1)
        head_sum = butterfly_sum(head_sum, "vocab", n)
        head_hit = jnp.arange(head_local, dtype=jnp.int32)[None, :] == head_aims[:, None]
        total = head_sum + clus_sum
        scale = factor / total
        kept_cap = lax.optimization_barrier(head_cap)
        head_pick = jnp.sum(jnp.where(head_hit, kept_cap, 0.0), 1)
        slope = 1.0 - (kept_cap * (1.0 / capping)) ** 2
        head_grad = (
            (jnp.exp(kept_cap) * scale[:, None] - jnp.where(head_hit, factor, 0.0)) * slope
        ).astype(bf16)
        clus_grad = (clus_exp * scale[:, None] - factor * clus_hit) * clus_slope
        head_terms = jnp.einsum("tv,fv->tf", head_grad, head_weight, preferred_element_type=f32)
        head_back = lax.psum_scatter(head_terms, "vocab", scatter_dimension=1, tiled=True)

        tail_caps, tail_hits, tail_sums, tail_picks = [None] * 3, [None] * 3, [None] * 3, [None] * 3
        for number in (1, 2, 0):
            out = outs[number]
            tail_cap = capped(
                jnp.dot(latents[number], out.astype(f32), precision=lax.Precision.HIGH)
            )
            aims = slot_aims[number * capacity : (number + 1) * capacity]
            aims = jnp.where(aims >= 0, aims, -1) - vocab_index * out.shape[1]
            aims = jnp.where(slot_aims[number * capacity : (number + 1) * capacity] >= 0, aims, -1)
            tail_hits[number] = jnp.arange(out.shape[1], dtype=jnp.int32)[None, :] == aims[:, None]
            tail_sums[number] = jnp.sum(jnp.exp(tail_cap), 1)
            tail_caps[number] = lax.optimization_barrier(tail_cap)
            tail_picks[number] = jnp.sum(jnp.where(tail_hits[number], tail_caps[number], 0.0), 1)
        tail_totals = butterfly_sum(jnp.concatenate(tail_sums), "vocab", n)
        tail_scales = factor * filled / tail_totals
        grad_parts = [None] * 3
        for number in (0, 1, 2):
            cap = tail_caps[number]
            tail_scale = tail_scales[number * capacity : (number + 1) * capacity]
            tail_grad = (
                (jnp.exp(cap) * tail_scale[:, None] - jnp.where(tail_hits[number], factor, 0.0))
                * (1.0 - (cap * (1.0 / capping)) ** 2)
            ).astype(bf16)
            grad_parts[number] = jnp.einsum(
                "sv,pv->sp", tail_grad, outs[number], preferred_element_type=f32
            )
        grad_one = halving_sum(grad_parts[0], "vocab", n, powers)
        grad_rest = halving_sum(jnp.concatenate([grad_parts[1], grad_parts[2]], 1), "vocab", n, turned)
        latent_grads = [grad_one, grad_rest[:, :width_two], grad_rest[:, width_two:]]
        tail_picks = butterfly_sum(jnp.concatenate(tail_picks), "vocab", n)

        backs = []
        for number in range(3):
            back = jnp.einsum(
                "sp,fp->sf",
                latent_grads[number],
                projs[number].astype(f32),
                precision=lax.Precision.HIGH,
            )
            backs.append(weights[number] * back)
        back = jnp.concatenate(backs, 0)
        back_top = lax.reduce_precision(back, 8, 7)
        back_rest = (back - back_top).astype(bf16)
        back_top = back_top.astype(bf16)
        pick_slots = functools.partial(jnp.einsum, "st,sf->tf", preferred_element_type=f32)
        tail_back = pick_slots(select, back_top) + pick_slots(select, back_rest)
        clus_rows = clus_rows.astype(f32)
        clus_back = (
            clus_grad[:, 0:1] * clus_rows[:, 0][None, :]
            + clus_grad[:, 1:2] * clus_rows[:, 1][None, :]
            + clus_grad[:, 2:3] * clus_rows[:, 2][None, :]
        )
        grads = head_back + (tail_back + clus_back)
        head_pick = butterfly_sum(head_pick, "vocab", n)
        head_loss = jnp.log(total) - head_pick - jnp.sum(clus_hit * clus_cap, 1)

    tail_loss = (jnp.log(tail_totals) - tail_picks) * filled
    slot_weights = jnp.repeat(weights, capacity)
    tail_loss = tail_loss * slot_weights
    token_loss = head_loss + jnp.sum(jnp.where(chosen, tail_loss[:, None], 0.0), 0)
    loss_sum = butterfly_sum(jnp.sum(token_loss)[None], "dp", groups)
    mean_loss = loss_sum[0] / all_tokens
    return (token_loss, mean_loss, grads)


def solution(mesh):
    body = functools.partial(per_device, mesh.shape["vocab"], mesh.shape["dp"])
    return jax.shard_map(
        body,
        mesh=mesh,
        in_specs=(
            P("dp", None),
            P("dp"),
            P("dp"),
            P(None, "vocab"),
            P(),
            P("vocab", None),
            P("vocab", None),
            P("vocab", None),
            P(None, "vocab"),
            P(None, "vocab"),
            P(None, "vocab"),
        ),
        out_specs=(P("dp"), P(), P("dp", "vocab")),
        check_vma=False,
    )
```

```python
import functools

import jax
import jax.numpy as jnp
from jax import lax
from jax.experimental import pallas as pl
from jax.experimental.pallas import tpu as pltpu
from jax.sharding import PartitionSpec as P


capping = 30.0
RING_LIMIT = 16
LOG2E = 1.4426950408889634


def capped(values):
    return capping * jnp.tanh(values * (1.0 / capping))


def butterfly_sum(values, axis, n):
    step = 1
    while step < n:
        pairs = [(i, i ^ step) for i in range(n)]
        other = lax.ppermute(values, axis, pairs)
        values = values + other
        step *= 2
    return values


def halving_sum(values, axis, n, steps):
    me = lax.axis_index(axis)
    bits = []
    for step in steps:
        bit = (me // step) % 2
        pairs = [(i, i ^ step) for i in range(n)]
        half = values.shape[0] // 2
        send = lax.dynamic_slice_in_dim(values, (1 - bit) * half, half, 0)
        keep = lax.dynamic_slice_in_dim(values, bit * half, half, 0)
        values = keep + lax.ppermute(send, axis, pairs)
        bits.append((bit, pairs))
    for bit, pairs in reversed(bits):
        other = lax.ppermute(values, axis, pairs)
        first = bit == 0
        values = jnp.concatenate(
            [jnp.where(first, values, other), jnp.where(first, other, values)], 0
        )
    return values


def dot_nt(a, b):
    return lax.dot_general(a, b, (((1,), (1,)), ((), ())), preferred_element_type=jnp.float32)


def block_width(words, most):
    width = most
    while words % width:
        width -= 128
    return width


def column_of(row):
    return jnp.transpose(jnp.broadcast_to(row, (128, row.shape[1])))[:, 0:1]


def peer_copy(source, target, send_sem, recv_sem, index, axis="vocab"):
    return pltpu.make_async_remote_copy(
        src_ref=source,
        dst_ref=target,
        send_sem=send_sem,
        recv_sem=recv_sem,
        device_id={axis: index},
        device_id_type=pl.DeviceIdType.MESH,
    )


def greet(n, me, groups, group):
    barrier = pltpu.get_barrier_semaphore()
    for step in range(1, groups):
        pl.semaphore_signal(
            barrier,
            inc=1,
            device_id={"dp": (group + step) % groups},
            device_id_type=pl.DeviceIdType.MESH,
        )
    for step in range(1, n):
        pl.semaphore_signal(
            barrier,
            inc=1,
            device_id={"vocab": (me + step) % n},
            device_id_type=pl.DeviceIdType.MESH,
        )
    return barrier


def group_of(n, me, rows_half):
    odd = me % 2
    line = me // 2
    rows_chunk = rows_half // (n // 2)
    own_half = pl.ds(pl.multiple_of(odd * rows_half, rows_half), rows_half)
    other_half = pl.ds(pl.multiple_of((1 - odd) * rows_half, rows_half), rows_half)

    def chunk(which):
        return pl.ds(pl.multiple_of(odd * rows_half + which * rows_chunk, rows_chunk), rows_chunk)

    return odd, line, me + 1 - 2 * odd, own_half, other_half, chunk


def scatter_phases(n, me, parts, refs):
    summed, half_in, chunk_in, half_send, half_recv, chunk_send, chunk_recv = refs
    lines = n // 2
    odd, line, partner, own_half, other_half, chunk = group_of(n, me, half_in.shape[0])

    def half_copy():
        return peer_copy(
            parts.at[other_half, :], half_in, half_send.at[0], half_recv.at[0], partner
        )

    def chunk_copy(step):
        peer = (line + step) % lines
        return peer_copy(
            summed.at[chunk(peer), :],
            chunk_in.at[step - 1],
            chunk_send.at[step - 1],
            chunk_recv.at[step - 1],
            2 * peer + odd,
        )

    def send_half():
        half_copy().start()

    def spread_chunks():
        half_copy().wait_recv()
        summed[own_half, :] = parts[own_half, :] + half_in[...]
        for step in range(1, lines):
            chunk_copy(step).start()

    def sum_chunks():
        whole = summed[chunk(line), :]
        for step in range(1, lines):
            chunk_copy(step).wait_recv()
            whole = whole + chunk_in[step - 1]
        return whole

    def drain():
        half_copy().wait_send()
        for step in range(1, lines):
            chunk_copy(step).wait_send()

    return send_half, spread_chunks, sum_chunks, drain


def gather_phases(n, me, refs):
    collected, half_send, half_recv, chunk_send, chunk_recv = refs
    lines = n // 2
    odd, line, partner, own_half, _, chunk = group_of(n, me, collected.shape[0] // 2)

    def half_copy():
        place = collected.at[own_half, :]
        return peer_copy(place, place, half_send.at[0], half_recv.at[0], partner)

    def chunk_copy(step):
        place = collected.at[chunk(line), :]
        return peer_copy(
            place,
            place,
            chunk_send.at[step - 1],
            chunk_recv.at[step - 1],
            2 * ((line + step) % lines) + odd,
        )

    def send_chunks(value):
        collected[chunk(line), :] = value
        for step in range(1, lines):
            chunk_copy(step).start()

    def swap_halves():
        for step in range(1, lines):
            chunk_copy(step).wait_recv()
        half_copy().start()

    def take_halves():
        half_copy().wait_recv()

    def drain():
        half_copy().wait_send()
        for step in range(1, lines):
            chunk_copy(step).wait_send()

    return send_chunks, swap_halves, take_halves, drain


def scatter_scratch(n, capacity, size):
    lines = n // 2
    dma = pltpu.SemaphoreType.DMA
    return [
        pltpu.VMEM((capacity, size), jnp.float32),
        pltpu.VMEM((capacity // 2, size), jnp.float32),
        pltpu.VMEM((lines - 1, capacity // 2 // lines, size), jnp.float32),
        dma((1,)),
        dma((1,)),
        dma((lines - 1,)),
        dma((lines - 1,)),
    ]


def gather_scratch(n, capacity, size):
    lines = n // 2
    dma = pltpu.SemaphoreType.DMA
    return [
        pltpu.VMEM((capacity, size), jnp.float32),
        dma((1,)),
        dma((1,)),
        dma((lines - 1,)),
        dma((lines - 1,)),
    ]


def split_pair(value):
    top = value.astype(jnp.bfloat16)
    return top, (value - top.astype(jnp.float32)).astype(jnp.bfloat16)


def spread_row(row):
    wide = jnp.broadcast_to(row.astype(jnp.float32), (128, row.shape[1]))
    return jnp.transpose(wide).astype(jnp.int32)


def share_row(n, me, stat_all, stat_send, stat_recv):
    def copy(step):
        return peer_copy(
            stat_all.at[me],
            stat_all.at[me],
            stat_send.at[step - 1],
            stat_recv.at[step - 1],
            (me + step) % n,
        )

    def send(sums, picks):
        sums = jnp.sum(jnp.transpose(sums), axis=0, keepdims=True)
        picks = jnp.sum(jnp.transpose(picks), axis=0, keepdims=True)
        line_of = lax.broadcasted_iota(jnp.int32, stat_all.shape[1:], 0)
        stat_all[me] = jnp.where(line_of == 0, sums, jnp.where(line_of == 1, picks, 0.0))
        for step in range(1, n):
            copy(step).start()

    def take():
        for step in range(1, n):
            copy(step).wait_recv()
        whole = stat_all[0]
        for index in range(1, n):
            whole = whole + stat_all[index]
        return whole

    def drain():
        for step in range(1, n):
            copy(step).wait_send()

    return send, take, drain


def share_groups(groups, group, held, send_sem, recv_sem):
    def copy(step):
        return peer_copy(
            held.at[group],
            held.at[group],
            send_sem.at[step - 1],
            recv_sem.at[step - 1],
            (group + step) % groups,
            "dp",
        )

    def send(value):
        held[group] = value
        for step in range(1, groups):
            copy(step).start()

    def take():
        for step in range(1, groups):
            copy(step).wait_recv()
        whole = held[0]
        for index in range(1, groups):
            whole = whole + held[index]
        return whole

    def drain():
        for step in range(1, groups):
            copy(step).wait_send()

    return send, take, drain


def head_kernel(
    n,
    groups,
    factor,
    hidden,
    table,
    cluster,
    proj_one,
    proj_two,
    proj_three,
    weight,
    grad,
    high,
    low,
    chunk_one,
    cluster_high,
    cluster_low,
    stats,
    weights,
    columns,
    ratios,
    sum_acc,
    pick_acc,
    stat_all,
    aims,
    parts_one,
    parts_rest,
    select,
    count_all,
    column_sem,
    stat_send,
    stat_recv,
    count_send,
    count_recv,
    *refs,
):
    f32, bf16 = jnp.float32, jnp.bfloat16
    me = lax.axis_index("vocab")
    group = lax.axis_index("dp")
    barrier = greet(n, me, groups, group)
    tokens = hidden.shape[0]
    wide = columns.shape[2]
    words = weight.shape[1]
    count = words // wide

    def fetch(i, slot):
        start = pl.multiple_of(i * wide, wide)
        return pltpu.make_async_copy(
            weight.at[:, pl.ds(start, wide)], columns.at[slot], column_sem.at[slot]
        )

    fetch(0, 0).start()
    capacity = tokens // 4
    width = proj_one.shape[0]
    slot_row = table[2:3, :]
    for base in range(0, 3 * capacity, capacity):
        slot = lax.broadcasted_iota(jnp.int32, (capacity, tokens), 0) + base
        select[base : base + capacity, :] = jnp.where(slot == slot_row, 1.0, 0.0).astype(bf16)
    own = pl.ds(pl.multiple_of(me * width, width), width)
    rows_all = jnp.dot(select[...], hidden[:, own], preferred_element_type=f32).astype(bf16)
    size_two = proj_two.shape[1]
    rest = parts_rest.shape[1]
    parts_one[...] = jnp.dot(rows_all[0:capacity], proj_one[...], preferred_element_type=f32)
    parts_rest[:, 0:size_two] = jnp.dot(
        rows_all[capacity : 2 * capacity], proj_two[...], preferred_element_type=f32
    )
    parts_rest[:, size_two:rest] = jnp.dot(
        rows_all[2 * capacity :], proj_three[...], preferred_element_type=f32
    )
    one_half, one_spread, one_sum, one_drain = scatter_phases(n, me, parts_one, refs[0:7])
    rest_half, rest_spread, rest_sum, rest_drain = scatter_phases(n, me, parts_rest, refs[7:14])
    rest_send, rest_swap, rest_take, rest_end = gather_phases(n, me, refs[14:19])
    send_stats, take_stats, drain_stats = share_row(n, me, stat_all, stat_send, stat_recv)
    send_counts, take_counts, drain_counts = share_groups(
        groups, group, count_all, count_send, count_recv
    )
    pl.semaphore_wait(barrier, n + groups - 2)
    rest_half()
    one_half()
    place = lax.broadcasted_iota(jnp.int32, (8, tokens), 0)
    marks = jnp.where(table[0:1, :] == place + 1, 1.0, 0.0)
    marks = jnp.sum(marks, axis=1, keepdims=True)
    send_counts(jnp.broadcast_to(marks, (8, 128)))

    labels = spread_row(table[0:1, :])
    targets = spread_row(table[1:2, :])
    lanes = lax.broadcasted_iota(jnp.int32, (tokens, 128), 1)
    aims[...] = jnp.where(labels == 0, targets, -1) - me * words
    first = jnp.where(me == 0, 1.0, 0.0)
    ratio = jnp.tanh(
        jnp.dot(hidden[...], cluster[...], preferred_element_type=f32) * (1.0 / capping)
    )
    power = jnp.exp(capping * ratio)
    sum_acc[...] = first * jnp.where(lanes < 3, power, 0.0)
    pick_acc[...] = first * jnp.where(lanes + 1 == labels, capping * ratio, 0.0)

    turns = [
        rest_spread,
        lambda: rest_send(rest_sum()),
        one_spread,
        rest_swap,
    ]
    rows_part = tokens // 2

    def body(i, carry):
        slot = i % 2
        fetch(i, slot).wait()

        @pl.when(i + 1 < count)
        def _():
            fetch(i + 1, 1 - slot).start()

        for turn, phase in enumerate(turns):

            @pl.when(i == min(1 + turn * count // (len(turns) + 1), count - 1))
            def _(phase=phase):
                phase()

        here = pl.multiple_of(i * wide, wide)
        for part in range(2):
            rows = pl.ds(part * rows_part, rows_part)
            values = jnp.dot(hidden[rows, :], columns[slot], preferred_element_type=f32)
            ratio = jnp.tanh(values * (1.0 / capping))
            ratios[rows, pl.ds(here, wide)] = ratio
            cap = capping * ratio
            power = jnp.exp(cap)
            aim = aims[rows, :] - here
            lane = lax.broadcasted_iota(jnp.int32, (rows_part, 128), 1)
            total = sum_acc[rows, :]
            pick = pick_acc[rows, :]
            for j in range(0, wide, 128):
                total = total + power[:, j : j + 128]
                pick = pick + jnp.where(lane + j == aim, cap[:, j : j + 128], 0.0)
            sum_acc[rows, :] = total
            pick_acc[rows, :] = pick
        return carry

    lax.fori_loop(0, count, body, 0)
    send_stats(sum_acc[...], pick_acc[...])
    whole = take_stats()
    stats[...] = whole
    sum_acc[...] = factor / jnp.transpose(jnp.broadcast_to(whole[0:1, :], (128, tokens)))
    step_rows = 64

    def finish(r, carry):
        rows = pl.ds(pl.multiple_of(r * step_rows, step_rows), step_rows)
        scale = sum_acc[rows, :]
        aim = aims[rows, :]
        lane = lax.broadcasted_iota(jnp.int32, (step_rows, 128), 1)
        for j in range(0, ratios.shape[1], 128):
            ratio = ratios[rows, j : j + 128]
            share = jnp.exp(capping * ratio) * scale
            share = share - jnp.where(lane + j == aim, factor, 0.0)
            grad[rows, j : j + 128] = (share * (1.0 - ratio * ratio)).astype(bf16)
        return carry

    lax.fori_loop(0, tokens // step_rows, finish, 0)
    share = power * sum_acc[...] - jnp.where(lanes + 1 == labels, factor, 0.0)
    share = jnp.where(lanes < 3, share * (1.0 - ratio * ratio), 0.0)
    cluster_high[...], cluster_low[...] = split_pair(share)
    amounts = take_counts()
    row_of = lax.broadcasted_iota(jnp.int32, (8, 128), 0)
    weights[...] = jnp.where(row_of < 3, groups * tokens / (4.0 * amounts), 0.0)
    drain_counts()
    chunk_one[...] = one_sum()
    rest_take()
    high[...], low[...] = split_pair(refs[14][...])
    one_drain()
    rest_drain()
    rest_end()
    drain_stats()


def head_forward(n, groups, factor, hidden, table, cluster, projs, weight):
    f32, bf16 = jnp.float32, jnp.bfloat16
    tokens, words = hidden.shape[0], weight.shape[1]
    capacity = tokens // 4
    size = projs[0].shape[1]
    rest = projs[1].shape[1] + projs[2].shape[1]
    wide = block_width(words, 256)
    vmem = pl.BlockSpec(memory_space=pltpu.VMEM)
    hbm = pl.BlockSpec(memory_space=pl.ANY)
    dma = pltpu.SemaphoreType.DMA
    return pl.pallas_call(
        functools.partial(head_kernel, n, groups, factor),
        out_shape=(
            jax.ShapeDtypeStruct((tokens, words), bf16),
            jax.ShapeDtypeStruct((capacity, rest), bf16),
            jax.ShapeDtypeStruct((capacity, rest), bf16),
            jax.ShapeDtypeStruct((capacity // n, size), f32),
            jax.ShapeDtypeStruct((tokens, 128), bf16),
            jax.ShapeDtypeStruct((tokens, 128), bf16),
            jax.ShapeDtypeStruct((8, tokens), f32),
            jax.ShapeDtypeStruct((8, 128), f32),
        ),
        in_specs=[vmem] * 6 + [hbm],
        out_specs=(vmem,) * 8,
        scratch_shapes=[
            pltpu.VMEM((2, weight.shape[0], wide), bf16),
            pltpu.VMEM((tokens, words), f32),
            pltpu.VMEM((tokens, 128), f32),
            pltpu.VMEM((tokens, 128), f32),
            pltpu.VMEM((n, 8, tokens), f32),
            pltpu.VMEM((tokens, 128), jnp.int32),
            pltpu.VMEM((capacity, size), f32),
            pltpu.VMEM((capacity, rest), f32),
            pltpu.VMEM((3 * capacity, tokens), bf16),
            pltpu.VMEM((groups, 8, 128), f32),
            dma((2,)),
            dma((n - 1,)),
            dma((n - 1,)),
            dma((groups - 1,)),
            dma((groups - 1,)),
        ]
        + scatter_scratch(n, capacity, size)
        + scatter_scratch(n, capacity, rest)
        + gather_scratch(n, capacity, rest),
        compiler_params=pltpu.CompilerParams(
            collective_id=1, has_side_effects=True, vmem_limit_bytes=60_000_000
        ),
    )(hidden, table, cluster, *projs, weight)


def ring_kernel(
    n,
    groups,
    factor,
    grad,
    table,
    high,
    low,
    chunk_one,
    cluster_high,
    cluster_low,
    cluster_rows,
    proj_one,
    proj_two,
    proj_three,
    weights,
    head_stats,
    weight,
    out_one,
    out_two,
    out_three,
    grads,
    losses,
    mean,
    blocks,
    ring,
    term,
    buf_one,
    buf_two,
    buf_three,
    mix,
    acc_one,
    acc_two,
    acc_three,
    sum_acc,
    pick_acc,
    stat_one,
    stat_rest,
    given_one,
    given_rest,
    high_one,
    low_one,
    aims,
    joins,
    backs,
    pair,
    tail_row,
    mean_all,
    block_sem,
    buf_sem,
    ring_send,
    ring_recv,
    stat_send,
    stat_recv,
    mean_send,
    mean_recv,
    *refs,
):
    f32, bf16 = jnp.float32, jnp.bfloat16
    me = lax.axis_index("vocab")
    half_n = n // 2
    odd = me % 2
    line = me // 2
    spot = (1 - odd) * line + odd * (n - 1 - line)

    def at(place):
        place = place % n
        back = place // half_n
        return (1 - back) * (2 * place) + back * (2 * (n - 1 - place) + 1)

    neighbour = (at(spot + 1), at(spot + n - 1))
    group = lax.axis_index("dp")
    barrier = greet(n, me, groups, group)
    width = blocks.shape[2]

    def block_copy(way, hop):
        place = at(spot + (n - 1 - hop if way == 0 else 1 + hop))
        start = pl.multiple_of(place * width, width)
        slot = hop % 2
        return pltpu.make_async_copy(
            weight.at[pl.ds(start, width), :], blocks.at[way, slot], block_sem.at[way, slot]
        )

    for hop in range(2):
        for way in range(2):
            block_copy(way, hop).start()

    capacity = high.shape[0]
    tokens = grad.shape[0]
    kinds = []
    size_two = out_two.shape[0]
    for number, (out, buf, acc, proj, tops, rests, given, span) in enumerate(
        (
            (out_one, buf_one, acc_one, proj_one, high_one, low_one, given_one, slice(None)),
            (out_two, buf_two, acc_two, proj_two, high, low, given_rest, slice(0, size_two)),
            (
                out_three,
                buf_three,
                acc_three,
                proj_three,
                high,
                low,
                given_rest,
                slice(size_two, high.shape[1]),
            ),
        )
    ):
        words = out.shape[1]
        wide = buf.shape[2]
        kinds.append(
            (number, span, out, buf, acc, words, wide, words // wide, proj, tops, rests, given)
        )

    def fetch(kind, i, slot):
        number, out, buf, wide = kind[0], kind[2], kind[3], kind[6]
        start = pl.multiple_of(i * wide, wide)
        source = out.at[:, pl.ds(start, wide)]
        if number < 2:
            return [pltpu.make_async_copy(source, buf.at[slot], buf_sem.at[number, slot])]
        size = out.shape[0]
        return [
            pltpu.make_async_copy(
                source, buf.at[slot, pl.ds(again * size, size), :], buf_sem.at[number + again, slot]
            )
            for again in range(2)
        ]

    for kind in kinds:
        for copy in fetch(kind, 0, 0):
            copy.start()
        acc = kind[4]
        acc[...] = jnp.zeros_like(acc)
    sum_acc[...] = jnp.zeros_like(sum_acc)
    pick_acc[...] = jnp.zeros_like(pick_acc)

    def tail_steps(kind, first, last):
        number, span, out, buf, acc, words, wide, count, _, tops, rests, _ = kind
        rows = pl.ds(number * capacity, capacity)

        def body(i, carry):
            slot = i % 2
            for copy in fetch(kind, i, slot):
                copy.wait()

            @pl.when(i + 1 < count)
            def _():
                for copy in fetch(kind, i + 1, 1 - slot):
                    copy.start()

            words_here = buf[slot]
            if number < 2:
                values = jnp.dot(tops[:, span], words_here, preferred_element_type=f32)
                values = values + jnp.dot(rests[:, span], words_here, preferred_element_type=f32)
            else:
                values = jnp.dot(pair[...], words_here, preferred_element_type=f32)
                words_here = buf[slot, 0 : acc.shape[1], :]
            aim = aims[rows, :] - me * words - i * wide
            total = sum_acc[rows, :]
            pick = pick_acc[rows, :]
            lane = lax.broadcasted_iota(jnp.int32, (capacity, 128), 1)
            for j in range(0, wide, 128):
                ratio = jnp.tanh(values[:, j : j + 128] * (1.0 / capping))
                power = jnp.exp2(ratio * (capping * LOG2E))
                hit = lane + j == aim
                total = total + power
                pick = pick + jnp.where(hit, ratio, 0.0)
                slope = 1.0 - ratio * ratio
                mix[0:capacity, j : j + 128] = jnp.where(hit, 0.0, power * slope).astype(bf16)
                mix[capacity : 2 * capacity, j : j + 128] = jnp.where(hit, 1.0, 0.0).astype(bf16)
            sum_acc[rows, :] = total
            pick_acc[rows, :] = pick
            acc[...] += dot_nt(mix[:, 0:wide], words_here)
            return carry

        lax.fori_loop(first, last, body, 0)

    one_stats = share_row(n, me, stat_one, stat_send.at[0], stat_recv.at[0])
    rest_stats = share_row(n, me, stat_rest, stat_send.at[1], stat_recv.at[1])
    latent_send, latent_swap, latent_take, latent_end = gather_phases(n, me, refs[0:5])
    one_half, one_spread, one_sum, one_drain = scatter_phases(n, me, given_one, refs[5:12])
    one_send, one_swap, one_take, one_end = gather_phases(n, me, refs[12:17])
    rest_half, rest_spread, rest_sum, rest_drain = scatter_phases(n, me, given_rest, refs[17:24])
    rest_send, rest_swap, rest_take, rest_end = gather_phases(n, me, refs[24:29])
    one, two, three = kinds

    def set_up():
        slot_row = table[2:3, :]
        target_row = table[1:2, :].astype(f32)
        for base in range(0, 3 * capacity, 128):
            slot = lax.broadcasted_iota(jnp.int32, (128, tokens), 0) + base
            found = jnp.where(slot == slot_row, target_row + 1.0, 0.0)
            found = jnp.sum(found, axis=1, keepdims=True) - 1.0
            aims[base : base + 128, :] = jnp.broadcast_to(found, (128, 128)).astype(jnp.int32)
        size = kinds[2][4].shape[1]
        pair[:, 0:size] = high[:, kinds[2][1]]
        pair[:, size : 2 * size] = low[:, kinds[2][1]]

    def join_slots():
        slots_here = spread_row(table[2:3, :])
        lanes = lax.broadcasted_iota(jnp.int32, (tokens, 128), 1)
        for base in range(0, 3 * capacity, 128):
            hit = lanes + base == slots_here
            joins[:, base : base + 128] = jnp.where(hit, 1.0, 0.0).astype(bf16)

    def take_latents():
        latent_take()
        high_one[...], low_one[...] = split_pair(refs[0][...])

    def share_stats(stats_of, first, last):
        rows = slice(first * capacity, last * capacity)
        stats_of[0](sum_acc[rows, :], capping * pick_acc[rows, :])

    def finish_stats(stats_of, group, send_half):
        whole = stats_of[1]()
        first = group[0][0]
        gap = jnp.log(whole[0:1, :]) - whole[1:2, :]
        for number, span, _, _, acc, words, _, _, _, _, _, given in group:
            rows = slice(number * capacity, (number + 1) * capacity)
            here = slice((number - first) * capacity, (number - first + 1) * capacity)
            total = column_of(whole[0:1, here])
            share = weights[number : number + 1, 0:1]
            tail_row[0:1, rows] = share * gap[:, here]
            ratio = jnp.sum(pick_acc[rows, :], axis=1, keepdims=True)
            pick = capping * ratio
            aim = aims[rows, 0:1]
            local = aim - me * words
            peak = (factor * (jnp.exp(pick) / total - 1.0) * (1.0 - ratio * ratio)).astype(bf16)
            inside = jnp.logical_and(local >= 0, local < words)
            peak = jnp.where(inside, peak.astype(f32), 0.0)
            scale = jnp.where(aim >= 0, factor / total, 0.0)
            given[:, span] = share * (
                scale * acc[0:capacity, :] + peak * acc[capacity : 2 * capacity, :]
            )
        send_half()

    def take_back(group, take, collected):
        take()
        for number, span, _, _, _, _, _, _, proj, _, _, _ in group:
            rows = slice(number * capacity, (number + 1) * capacity)
            top, lower = split_pair(collected[:, span])
            back = dot_nt(top, proj[...]) + dot_nt(lower, proj[...])
            backs[0, rows, :], backs[1, rows, :] = split_pair(back)

    send_mean, take_mean, drain_mean = share_groups(groups, group, mean_all, mean_send, mean_recv)

    def token_losses():
        tails = tail_row[0:1, :]
        total = jnp.zeros((tokens, 128), f32)
        for base in range(0, 3 * capacity, 128):
            total = total + joins[:, base : base + 128].astype(f32) * tails[:, base : base + 128]
        tail = jnp.sum(jnp.transpose(total), axis=0, keepdims=True)
        value = jnp.log(head_stats[0:1, :]) - head_stats[1:2, :] + tail
        losses[...] = jnp.broadcast_to(value, (8, tokens))
        send_mean(jnp.broadcast_to(jnp.sum(value, axis=1, keepdims=True), (8, 128)))

    def mean_loss():
        mean[...] = take_mean() * (1.0 / (groups * tokens))

    def join_backs():
        total = jnp.dot(joins[...], backs[0], preferred_element_type=f32)
        total = total + jnp.dot(joins[...], backs[1], preferred_element_type=f32)
        total = total + jnp.dot(cluster_high[...], cluster_rows[...], preferred_element_type=f32)
        grads[...] = total + jnp.dot(
            cluster_low[...], cluster_rows[...], preferred_element_type=f32
        )

    rows_way = grad.shape[0] // 2
    rows_part = rows_way // 2

    def product(way, hop):
        block_copy(way, hop).wait()
        part = grad[way * rows_way : (way + 1) * rows_way, :]
        return dot_nt(part, blocks[way, hop % 2])

    def next_block(way, hop):
        if hop + 2 < n:
            block_copy(way, hop + 2).start()

    def hop_copy(way, part, hop):
        rows = pl.ds(part * rows_part, rows_part)
        return peer_copy(
            ring.at[way, hop, rows, :],
            ring.at[way, hop + 1, rows, :],
            ring_send.at[way, part, hop],
            ring_recv.at[way, part, hop],
            neighbour[way],
        )

    def tails(kind, first, last):
        count = kind[7]
        return functools.partial(
            tail_steps, kind, int(count * first + 0.5), int(count * last + 0.5)
        )

    bind = functools.partial
    plan = [
        [set_up, tails(three, 0, 5 / 18)],
        [latent_swap, tails(three, 5 / 18, 9 / 18)],
        [tails(three, 9 / 18, 15 / 18)],
        [tails(three, 15 / 18, 1), take_latents, tails(two, 0, 2 / 8)],
        [tails(two, 2 / 8, 1), bind(share_stats, rest_stats, 1, 3)],
        [bind(finish_stats, rest_stats, (two, three), rest_half), tails(one, 0, 2 / 4)],
        [rest_spread, tails(one, 2 / 4, 1), bind(share_stats, one_stats, 0, 1)],
        [
            bind(finish_stats, one_stats, (one,), one_half),
            lambda: rest_send(rest_sum()),
        ],
        [one_spread, rest_swap, join_slots, token_losses],
        [lambda: one_send(one_sum()), bind(take_back, (two, three), rest_take, refs[24])],
        [one_swap, mean_loss],
        [bind(take_back, (one,), one_take, refs[12]), join_backs],
    ]
    work = [[] for _ in range(2 * (n - 1))]
    for i, group in enumerate(plan):
        work[i * (len(work) - 2) // len(plan)] += group

    pl.semaphore_wait(barrier, n + groups - 2)
    for way in range(2):
        ring[way, 0] = product(way, 0)
        next_block(way, 0)
        for part in range(2):
            hop_copy(way, part, 0).start()
    latent_send(chunk_one[...])
    for way in range(2):
        term[way] = product(way, 1)
        next_block(way, 1)
    for hop in range(n - 1):
        for part in range(2):
            rows = pl.ds(part * rows_part, rows_part)
            for way in range(2):
                hop_copy(way, part, hop).wait_recv()
                held = ring[way, hop + 1, rows, :] + term[way, rows, :]
                if hop < n - 2:
                    ring[way, hop + 1, rows, :] = held
                    hop_copy(way, part, hop + 1).start()
                else:
                    grads[pl.ds(way * rows_way + part * rows_part, rows_part), :] += held
            if part == 1 and hop < n - 2:
                for way in range(2):
                    term[way] = product(way, hop + 2)
                    next_block(way, hop + 2)
            for piece in work[2 * hop + part]:
                piece()
    for way in range(2):
        for part in range(2):
            for hop in range(n - 1):
                hop_copy(way, part, hop).wait_send()
    one_stats[2]()
    rest_stats[2]()
    drain_mean()
    latent_end()
    one_drain()
    one_end()
    rest_drain()
    rest_end()


def ring_and_tails(
    n, groups, factor, grad, table, latents, clusters, projs, weights, head_stats, weight, outs
):
    f32, bf16 = jnp.float32, jnp.bfloat16
    tokens = grad.shape[0]
    capacity = latents[0].shape[0]
    width = projs[0].shape[0]
    rest = latents[0].shape[1]
    sizes = [out.shape[0] for out in outs]
    wides = [block_width(out.shape[1], 1024) for out in outs]
    vmem = pl.BlockSpec(memory_space=pltpu.VMEM)
    hbm = pl.BlockSpec(memory_space=pl.ANY)
    dma = pltpu.SemaphoreType.DMA
    return pl.pallas_call(
        functools.partial(ring_kernel, n, groups, factor),
        out_shape=(
            jax.ShapeDtypeStruct((tokens, width), f32),
            jax.ShapeDtypeStruct((8, tokens), f32),
            jax.ShapeDtypeStruct((8, 128), f32),
        ),
        in_specs=[vmem] * 13 + [hbm] * 4,
        out_specs=(vmem, vmem, vmem),
        scratch_shapes=[
            pltpu.VMEM((2, 2, width, weight.shape[1]), bf16),
            pltpu.VMEM((2, n, tokens // 2, width), f32),
            pltpu.VMEM((2, tokens // 2, width), f32),
        ]
        + [
            pltpu.VMEM((2, times * size, wide), bf16)
            for times, size, wide in zip((1, 1, 2), sizes, wides)
        ]
        + [pltpu.VMEM((2 * capacity, max(wides)), bf16)]
        + [pltpu.VMEM((2 * capacity, size), f32) for size in sizes]
        + [
            pltpu.VMEM((3 * capacity, 128), f32),
            pltpu.VMEM((3 * capacity, 128), f32),
            pltpu.VMEM((n, 8, capacity), f32),
            pltpu.VMEM((n, 8, 2 * capacity), f32),
            pltpu.VMEM((capacity, sizes[0]), f32),
            pltpu.VMEM((capacity, rest), f32),
            pltpu.VMEM((capacity, sizes[0]), bf16),
            pltpu.VMEM((capacity, sizes[0]), bf16),
            pltpu.VMEM((3 * capacity, 128), jnp.int32),
            pltpu.VMEM((tokens, 3 * capacity), bf16),
            pltpu.VMEM((2, 3 * capacity, width), bf16),
            pltpu.VMEM((capacity, 2 * sizes[2]), bf16),
            pltpu.VMEM((8, 3 * capacity), f32),
            pltpu.VMEM((groups, 8, 128), f32),
            dma((2, 2)),
            dma((4, 2)),
            dma((2, 2, n - 1)),
            dma((2, 2, n - 1)),
            dma((2, n - 1)),
            dma((2, n - 1)),
            dma((groups - 1,)),
            dma((groups - 1,)),
        ]
        + gather_scratch(n, capacity, sizes[0])
        + scatter_scratch(n, capacity, sizes[0])
        + gather_scratch(n, capacity, sizes[0])
        + scatter_scratch(n, capacity, rest)
        + gather_scratch(n, capacity, rest),
        compiler_params=pltpu.CompilerParams(
            collective_id=0, has_side_effects=True, vmem_limit_bytes=66_000_000
        ),
    )(grad, table, *latents, *clusters, *projs, weights, head_stats, weight, *outs)


def per_device(
    n,
    groups,
    hidden,
    labels,
    targets,
    head_weight,
    cluster_weight,
    proj_one,
    proj_two,
    proj_three,
    out_one,
    out_two,
    out_three,
):
    f32, bf16 = jnp.float32, jnp.bfloat16
    tokens = hidden.shape[0]
    width = proj_one.shape[0]
    head_local = head_weight.shape[1]
    capacity = tokens // 4
    all_tokens = tokens * groups
    vocab_index = lax.axis_index("vocab")
    feat_start = vocab_index * width
    factor = jnp.sqrt(f32(hidden.shape[1]))
    projs = (proj_one, proj_two, proj_three)
    outs = (out_one, out_two, out_three)

    member = labels[None, :] == jnp.arange(1, 4, dtype=jnp.int32)[:, None]
    local_counts = jnp.sum(member.astype(f32), 1)
    row = jnp.arange(tokens, dtype=jnp.int32)
    upto = (row[:, None] <= row[None, :]).astype(bf16)
    placed = jnp.dot(member.astype(bf16), upto, preferred_element_type=f32).astype(jnp.int32) - 1
    offsets = jnp.arange(3, dtype=jnp.int32)[:, None] * capacity
    slot_of = jnp.sum(jnp.where(member, placed + offsets + 1, 0), 0) - 1
    slot_ids = jnp.arange(3 * capacity, dtype=jnp.int32)
    chosen = slot_ids[:, None] == slot_of[None, :]
    select = chosen.astype(bf16)
    slot_aims = jnp.sum(jnp.where(chosen, targets[None, :] + 1, 0), 1) - 1
    filled = (slot_aims >= 0).astype(f32)

    own_features = lax.dynamic_slice_in_dim(hidden, feat_start, width, 1)
    picked_rows = jnp.dot(select, own_features, preferred_element_type=f32).astype(bf16)
    latent_parts = []
    for number in range(3):
        chunk = picked_rows[number * capacity : (number + 1) * capacity]
        latent_parts.append(jnp.dot(chunk, projs[number], preferred_element_type=f32))
    counts = butterfly_sum(local_counts, "dp", groups)
    weights = all_tokens / (4.0 * counts)
    clus_cap = capped(jnp.dot(hidden, cluster_weight, preferred_element_type=f32))
    clus_exp = jnp.exp(clus_cap)
    clus_hit = (jnp.arange(3, dtype=jnp.int32)[None, :] + 1 == labels[:, None]).astype(f32)
    clus_sum = jnp.sum(clus_exp, 1)
    clus_slope = 1.0 - (clus_cap * (1.0 / capping)) ** 2
    head_aims = jnp.where(labels == 0, targets, -1) - vocab_index * head_local
    clus_rows = lax.dynamic_slice_in_dim(cluster_weight, feat_start, width, 0)

    if n <= RING_LIMIT:
        scale_of = float(hidden.shape[1]) ** 0.5
        table = jnp.concatenate(
            [
                jnp.stack([labels, targets, slot_of]),
                jnp.zeros((5, tokens), jnp.int32),
            ],
            0,
        )
        padded = jnp.pad(cluster_weight, ((0, 0), (0, 125)))
        grad, high, low, chunk, clus_high, clus_low, head_stats, weights = head_forward(
            n, groups, scale_of, hidden, table, padded, projs, head_weight
        )
        clus_lines = jnp.pad(jnp.transpose(clus_rows), ((0, 125), (0, 0)))
        grads, losses, mean = ring_and_tails(
            n,
            groups,
            scale_of,
            grad,
            table,
            (high, low, chunk),
            (clus_high, clus_low, clus_lines),
            projs,
            weights,
            head_stats,
            head_weight,
            outs,
        )
        return (losses[0], mean[0, 0], grads)
    else:
        powers = []
        step = 1
        while step < n:
            powers.append(step)
            step *= 2
        turned = powers[1:] + powers[:1]
        joined = jnp.concatenate([latent_parts[1], latent_parts[2]], 1)
        joined = halving_sum(joined, "vocab", n, turned)
        width_two = projs[1].shape[1]
        latents = [
            halving_sum(latent_parts[0], "vocab", n, powers),
            joined[:, :width_two],
            joined[:, width_two:],
        ]
        head_cap = capped(jnp.dot(hidden, head_weight, preferred_element_type=f32))
        head_sum = jnp.sum(jnp.exp(head_cap), 1)
        head_sum = butterfly_sum(head_sum, "vocab", n)
        head_hit = jnp.arange(head_local, dtype=jnp.int32)[None, :] == head_aims[:, None]
        total = head_sum + clus_sum
        scale = factor / total
        kept_cap = lax.optimization_barrier(head_cap)
        head_pick = jnp.sum(jnp.where(head_hit, kept_cap, 0.0), 1)
        slope = 1.0 - (kept_cap * (1.0 / capping)) ** 2
        head_grad = (
            (jnp.exp(kept_cap) * scale[:, None] - jnp.where(head_hit, factor, 0.0)) * slope
        ).astype(bf16)
        clus_grad = (clus_exp * scale[:, None] - factor * clus_hit) * clus_slope
        head_terms = jnp.einsum("tv,fv->tf", head_grad, head_weight, preferred_element_type=f32)
        head_back = lax.psum_scatter(head_terms, "vocab", scatter_dimension=1, tiled=True)

        tail_caps, tail_hits, tail_sums, tail_picks = [None] * 3, [None] * 3, [None] * 3, [None] * 3
        for number in (1, 2, 0):
            out = outs[number]
            tail_cap = capped(
                jnp.dot(latents[number], out.astype(f32), precision=lax.Precision.HIGH)
            )
            aims = slot_aims[number * capacity : (number + 1) * capacity]
            aims = jnp.where(aims >= 0, aims, -1) - vocab_index * out.shape[1]
            aims = jnp.where(slot_aims[number * capacity : (number + 1) * capacity] >= 0, aims, -1)
            tail_hits[number] = jnp.arange(out.shape[1], dtype=jnp.int32)[None, :] == aims[:, None]
            tail_sums[number] = jnp.sum(jnp.exp(tail_cap), 1)
            tail_caps[number] = lax.optimization_barrier(tail_cap)
            tail_picks[number] = jnp.sum(jnp.where(tail_hits[number], tail_caps[number], 0.0), 1)
        tail_totals = butterfly_sum(jnp.concatenate(tail_sums), "vocab", n)
        tail_scales = factor * filled / tail_totals
        grad_parts = [None] * 3
        for number in (0, 1, 2):
            cap = tail_caps[number]
            tail_scale = tail_scales[number * capacity : (number + 1) * capacity]
            tail_grad = (
                (jnp.exp(cap) * tail_scale[:, None] - jnp.where(tail_hits[number], factor, 0.0))
                * (1.0 - (cap * (1.0 / capping)) ** 2)
            ).astype(bf16)
            grad_parts[number] = jnp.einsum(
                "sv,pv->sp", tail_grad, outs[number], preferred_element_type=f32
            )
        grad_one = halving_sum(grad_parts[0], "vocab", n, powers)
        grad_rest = halving_sum(jnp.concatenate([grad_parts[1], grad_parts[2]], 1), "vocab", n, turned)
        latent_grads = [grad_one, grad_rest[:, :width_two], grad_rest[:, width_two:]]
        tail_picks = butterfly_sum(jnp.concatenate(tail_picks), "vocab", n)

        backs = []
        for number in range(3):
            back = jnp.einsum(
                "sp,fp->sf",
                latent_grads[number],
                projs[number].astype(f32),
                precision=lax.Precision.HIGH,
            )
            backs.append(weights[number] * back)
        back = jnp.concatenate(backs, 0)
        back_top = lax.reduce_precision(back, 8, 7)
        back_rest = (back - back_top).astype(bf16)
        back_top = back_top.astype(bf16)
        pick_slots = functools.partial(jnp.einsum, "st,sf->tf", preferred_element_type=f32)
        tail_back = pick_slots(select, back_top) + pick_slots(select, back_rest)
        clus_rows = clus_rows.astype(f32)
        clus_back = (
            clus_grad[:, 0:1] * clus_rows[:, 0][None, :]
            + clus_grad[:, 1:2] * clus_rows[:, 1][None, :]
            + clus_grad[:, 2:3] * clus_rows[:, 2][None, :]
        )
        grads = head_back + (tail_back + clus_back)
        head_pick = butterfly_sum(head_pick, "vocab", n)
        head_loss = jnp.log(total) - head_pick - jnp.sum(clus_hit * clus_cap, 1)

    tail_loss = (jnp.log(tail_totals) - tail_picks) * filled
    slot_weights = jnp.repeat(weights, capacity)
    tail_loss = tail_loss * slot_weights
    token_loss = head_loss + jnp.sum(jnp.where(chosen, tail_loss[:, None], 0.0), 0)
    loss_sum = butterfly_sum(jnp.sum(token_loss)[None], "dp", groups)
    mean_loss = loss_sum[0] / all_tokens
    return (token_loss, mean_loss, grads)


def solution(mesh):
    body = functools.partial(per_device, mesh.shape["vocab"], mesh.shape["dp"])
    return jax.shard_map(
        body,
        mesh=mesh,
        in_specs=(
            P("dp", None),
            P("dp"),
            P("dp"),
            P(None, "vocab"),
            P(),
            P("vocab", None),
            P("vocab", None),
            P("vocab", None),
            P(None, "vocab"),
            P(None, "vocab"),
            P(None, "vocab"),
        ),
        out_specs=(P("dp"), P(), P("dp", "vocab")),
        check_vma=False,
    )
```

```python
import functools

import jax
import jax.numpy as jnp
from jax import lax
from jax.experimental import pallas as pl
from jax.experimental.pallas import tpu as pltpu
from jax.sharding import PartitionSpec as P


capping = 30.0
RING_LIMIT = 16
LOG2E = 1.4426950408889634


def capped(values):
    return capping * jnp.tanh(values * (1.0 / capping))


def butterfly_sum(values, axis, n):
    step = 1
    while step < n:
        pairs = [(i, i ^ step) for i in range(n)]
        other = lax.ppermute(values, axis, pairs)
        values = values + other
        step *= 2
    return values


def halving_sum(values, axis, n, steps):
    me = lax.axis_index(axis)
    bits = []
    for step in steps:
        bit = (me // step) % 2
        pairs = [(i, i ^ step) for i in range(n)]
        half = values.shape[0] // 2
        send = lax.dynamic_slice_in_dim(values, (1 - bit) * half, half, 0)
        keep = lax.dynamic_slice_in_dim(values, bit * half, half, 0)
        values = keep + lax.ppermute(send, axis, pairs)
        bits.append((bit, pairs))
    for bit, pairs in reversed(bits):
        other = lax.ppermute(values, axis, pairs)
        first = bit == 0
        values = jnp.concatenate(
            [jnp.where(first, values, other), jnp.where(first, other, values)], 0
        )
    return values


def dot_nt(a, b):
    return lax.dot_general(a, b, (((1,), (1,)), ((), ())), preferred_element_type=jnp.float32)


def block_width(words, most):
    width = most
    while words % width:
        width -= 128
    return width


def column_of(row):
    return jnp.transpose(jnp.broadcast_to(row, (128, row.shape[1])))[:, 0:1]


def peer_copy(source, target, send_sem, recv_sem, index, axis="vocab"):
    return pltpu.make_async_remote_copy(
        src_ref=source,
        dst_ref=target,
        send_sem=send_sem,
        recv_sem=recv_sem,
        device_id={axis: index},
        device_id_type=pl.DeviceIdType.MESH,
    )


def greet(n, me, groups, group):
    barrier = pltpu.get_barrier_semaphore()
    for step in range(1, groups):
        pl.semaphore_signal(
            barrier,
            inc=1,
            device_id={"dp": (group + step) % groups},
            device_id_type=pl.DeviceIdType.MESH,
        )
    for step in range(1, n):
        pl.semaphore_signal(
            barrier,
            inc=1,
            device_id={"vocab": (me + step) % n},
            device_id_type=pl.DeviceIdType.MESH,
        )
    return barrier


def group_of(n, me, rows_half):
    odd = me % 2
    line = me // 2
    rows_chunk = rows_half // (n // 2)
    own_half = pl.ds(pl.multiple_of(odd * rows_half, rows_half), rows_half)
    other_half = pl.ds(pl.multiple_of((1 - odd) * rows_half, rows_half), rows_half)

    def chunk(which):
        return pl.ds(pl.multiple_of(odd * rows_half + which * rows_chunk, rows_chunk), rows_chunk)

    return odd, line, me + 1 - 2 * odd, own_half, other_half, chunk


def scatter_phases(n, me, parts, refs):
    summed, half_in, chunk_in, half_send, half_recv, chunk_send, chunk_recv = refs
    lines = n // 2
    odd, line, partner, own_half, other_half, chunk = group_of(n, me, half_in.shape[0])

    def half_copy():
        return peer_copy(
            parts.at[other_half, :], half_in, half_send.at[0], half_recv.at[0], partner
        )

    def chunk_copy(step):
        peer = (line + step) % lines
        return peer_copy(
            summed.at[chunk(peer), :],
            chunk_in.at[step - 1],
            chunk_send.at[step - 1],
            chunk_recv.at[step - 1],
            2 * peer + odd,
        )

    def send_half():
        half_copy().start()

    def spread_chunks():
        half_copy().wait_recv()
        summed[own_half, :] = parts[own_half, :] + half_in[...]
        for step in range(1, lines):
            chunk_copy(step).start()

    def sum_chunks():
        whole = summed[chunk(line), :]
        for step in range(1, lines):
            chunk_copy(step).wait_recv()
            whole = whole + chunk_in[step - 1]
        return whole

    def drain():
        half_copy().wait_send()
        for step in range(1, lines):
            chunk_copy(step).wait_send()

    return send_half, spread_chunks, sum_chunks, drain


def gather_phases(n, me, refs):
    collected, half_send, half_recv, chunk_send, chunk_recv = refs
    lines = n // 2
    odd, line, partner, own_half, _, chunk = group_of(n, me, collected.shape[0] // 2)

    def half_copy():
        place = collected.at[own_half, :]
        return peer_copy(place, place, half_send.at[0], half_recv.at[0], partner)

    def chunk_copy(step):
        place = collected.at[chunk(line), :]
        return peer_copy(
            place,
            place,
            chunk_send.at[step - 1],
            chunk_recv.at[step - 1],
            2 * ((line + step) % lines) + odd,
        )

    def send_chunks(value):
        collected[chunk(line), :] = value
        for step in range(1, lines):
            chunk_copy(step).start()

    def swap_halves():
        for step in range(1, lines):
            chunk_copy(step).wait_recv()
        half_copy().start()

    def take_halves():
        half_copy().wait_recv()

    def drain():
        half_copy().wait_send()
        for step in range(1, lines):
            chunk_copy(step).wait_send()

    return send_chunks, swap_halves, take_halves, drain


def scatter_scratch(n, capacity, size):
    lines = n // 2
    dma = pltpu.SemaphoreType.DMA
    return [
        pltpu.VMEM((capacity, size), jnp.float32),
        pltpu.VMEM((capacity // 2, size), jnp.float32),
        pltpu.VMEM((lines - 1, capacity // 2 // lines, size), jnp.float32),
        dma((1,)),
        dma((1,)),
        dma((lines - 1,)),
        dma((lines - 1,)),
    ]


def gather_scratch(n, capacity, size):
    lines = n // 2
    dma = pltpu.SemaphoreType.DMA
    return [
        pltpu.VMEM((capacity, size), jnp.float32),
        dma((1,)),
        dma((1,)),
        dma((lines - 1,)),
        dma((lines - 1,)),
    ]


def split_pair(value):
    top = value.astype(jnp.bfloat16)
    return top, (value - top.astype(jnp.float32)).astype(jnp.bfloat16)


def spread_row(row):
    wide = jnp.broadcast_to(row.astype(jnp.float32), (128, row.shape[1]))
    return jnp.transpose(wide).astype(jnp.int32)


def share_row(n, me, stat_all, stat_send, stat_recv):
    def copy(step):
        return peer_copy(
            stat_all.at[me],
            stat_all.at[me],
            stat_send.at[step - 1],
            stat_recv.at[step - 1],
            (me + step) % n,
        )

    def send(sums, picks):
        sums = jnp.sum(jnp.transpose(sums), axis=0, keepdims=True)
        picks = jnp.sum(jnp.transpose(picks), axis=0, keepdims=True)
        line_of = lax.broadcasted_iota(jnp.int32, stat_all.shape[1:], 0)
        stat_all[me] = jnp.where(line_of == 0, sums, jnp.where(line_of == 1, picks, 0.0))
        for step in range(1, n):
            copy(step).start()

    def take():
        for step in range(1, n):
            copy(step).wait_recv()
        whole = stat_all[0]
        for index in range(1, n):
            whole = whole + stat_all[index]
        return whole

    def drain():
        for step in range(1, n):
            copy(step).wait_send()

    return send, take, drain


def share_groups(groups, group, held, send_sem, recv_sem):
    def copy(step):
        return peer_copy(
            held.at[group],
            held.at[group],
            send_sem.at[step - 1],
            recv_sem.at[step - 1],
            (group + step) % groups,
            "dp",
        )

    def send(value):
        held[group] = value
        for step in range(1, groups):
            copy(step).start()

    def take():
        for step in range(1, groups):
            copy(step).wait_recv()
        whole = held[0]
        for index in range(1, groups):
            whole = whole + held[index]
        return whole

    def drain():
        for step in range(1, groups):
            copy(step).wait_send()

    return send, take, drain


def head_kernel(
    n,
    groups,
    factor,
    hidden,
    table,
    cluster,
    proj_one,
    proj_two,
    proj_three,
    weight,
    grad,
    high,
    low,
    chunk_one,
    cluster_high,
    cluster_low,
    stats,
    weights,
    columns,
    ratios,
    sum_acc,
    pick_acc,
    stat_all,
    aims,
    parts_one,
    parts_rest,
    select,
    count_all,
    column_sem,
    stat_send,
    stat_recv,
    count_send,
    count_recv,
    *refs,
):
    f32, bf16 = jnp.float32, jnp.bfloat16
    me = lax.axis_index("vocab")
    group = lax.axis_index("dp")
    barrier = greet(n, me, groups, group)
    tokens = hidden.shape[0]
    wide = columns.shape[2]
    words = weight.shape[1]
    count = words // wide

    def fetch(i, slot):
        start = pl.multiple_of(i * wide, wide)
        return pltpu.make_async_copy(
            weight.at[:, pl.ds(start, wide)], columns.at[slot], column_sem.at[slot]
        )

    fetch(0, 0).start()
    capacity = tokens // 4
    width = proj_one.shape[0]
    slot_row = table[2:3, :]
    for base in range(0, 3 * capacity, capacity):
        slot = lax.broadcasted_iota(jnp.int32, (capacity, tokens), 0) + base
        select[base : base + capacity, :] = jnp.where(slot == slot_row, 1.0, 0.0).astype(bf16)
    own = pl.ds(pl.multiple_of(me * width, width), width)
    rows_all = jnp.dot(select[...], hidden[:, own], preferred_element_type=f32).astype(bf16)
    size_two = proj_two.shape[1]
    rest = parts_rest.shape[1]
    parts_one[...] = jnp.dot(rows_all[0:capacity], proj_one[...], preferred_element_type=f32)
    parts_rest[:, 0:size_two] = jnp.dot(
        rows_all[capacity : 2 * capacity], proj_two[...], preferred_element_type=f32
    )
    parts_rest[:, size_two:rest] = jnp.dot(
        rows_all[2 * capacity :], proj_three[...], preferred_element_type=f32
    )
    one_half, one_spread, one_sum, one_drain = scatter_phases(n, me, parts_one, refs[0:7])
    rest_half, rest_spread, rest_sum, rest_drain = scatter_phases(n, me, parts_rest, refs[7:14])
    rest_send, rest_swap, rest_take, rest_end = gather_phases(n, me, refs[14:19])
    send_stats, take_stats, drain_stats = share_row(n, me, stat_all, stat_send, stat_recv)
    send_counts, take_counts, drain_counts = share_groups(
        groups, group, count_all, count_send, count_recv
    )
    pl.semaphore_wait(barrier, n + groups - 2)
    rest_half()
    one_half()
    place = lax.broadcasted_iota(jnp.int32, (8, tokens), 0)
    marks = jnp.where(table[0:1, :] == place + 1, 1.0, 0.0)
    marks = jnp.sum(marks, axis=1, keepdims=True)
    send_counts(jnp.broadcast_to(marks, (8, 128)))

    labels = spread_row(table[0:1, :])
    targets = spread_row(table[1:2, :])
    lanes = lax.broadcasted_iota(jnp.int32, (tokens, 128), 1)
    aims[...] = jnp.where(labels == 0, targets, -1) - me * words
    first = jnp.where(me == 0, 1.0, 0.0)
    ratio = jnp.tanh(
        jnp.dot(hidden[...], cluster[...], preferred_element_type=f32) * (1.0 / capping)
    )
    power = jnp.exp(capping * ratio)
    sum_acc[...] = first * jnp.where(lanes < 3, power, 0.0)
    pick_acc[...] = first * jnp.where(lanes + 1 == labels, capping * ratio, 0.0)

    turns = [
        rest_spread,
        lambda: rest_send(rest_sum()),
        one_spread,
        rest_swap,
    ]
    rows_part = tokens // 2

    def body(i, carry):
        slot = i % 2
        fetch(i, slot).wait()

        @pl.when(i + 1 < count)
        def _():
            fetch(i + 1, 1 - slot).start()

        for turn, phase in enumerate(turns):

            @pl.when(i == min(1 + turn * count // (len(turns) + 1), count - 1))
            def _(phase=phase):
                phase()

        here = pl.multiple_of(i * wide, wide)
        for part in range(2):
            rows = pl.ds(part * rows_part, rows_part)
            values = jnp.dot(hidden[rows, :], columns[slot], preferred_element_type=f32)
            ratio = jnp.tanh(values * (1.0 / capping))
            ratios[rows, pl.ds(here, wide)] = ratio
            cap = capping * ratio
            power = jnp.exp(cap)
            aim = aims[rows, :] - here
            lane = lax.broadcasted_iota(jnp.int32, (rows_part, 128), 1)
            total = sum_acc[rows, :]
            pick = pick_acc[rows, :]
            for j in range(0, wide, 128):
                total = total + power[:, j : j + 128]
                pick = pick + jnp.where(lane + j == aim, cap[:, j : j + 128], 0.0)
            sum_acc[rows, :] = total
            pick_acc[rows, :] = pick
        return carry

    lax.fori_loop(0, count, body, 0)
    send_stats(sum_acc[...], pick_acc[...])
    whole = take_stats()
    stats[...] = whole
    sum_acc[...] = factor / jnp.transpose(jnp.broadcast_to(whole[0:1, :], (128, tokens)))
    step_rows = 64

    def finish(r, carry):
        rows = pl.ds(pl.multiple_of(r * step_rows, step_rows), step_rows)
        scale = sum_acc[rows, :]
        aim = aims[rows, :]
        lane = lax.broadcasted_iota(jnp.int32, (step_rows, 128), 1)
        for j in range(0, ratios.shape[1], 128):
            ratio = ratios[rows, j : j + 128]
            share = jnp.exp(capping * ratio) * scale
            share = share - jnp.where(lane + j == aim, factor, 0.0)
            grad[rows, j : j + 128] = (share * (1.0 - ratio * ratio)).astype(bf16)
        return carry

    lax.fori_loop(0, tokens // step_rows, finish, 0)
    share = power * sum_acc[...] - jnp.where(lanes + 1 == labels, factor, 0.0)
    share = jnp.where(lanes < 3, share * (1.0 - ratio * ratio), 0.0)
    cluster_high[...], cluster_low[...] = split_pair(share)
    amounts = take_counts()
    row_of = lax.broadcasted_iota(jnp.int32, (8, 128), 0)
    weights[...] = jnp.where(row_of < 3, groups * tokens / (4.0 * amounts), 0.0)
    drain_counts()
    chunk_one[...] = one_sum()
    rest_take()
    high[...], low[...] = split_pair(refs[14][...])
    one_drain()
    rest_drain()
    rest_end()
    drain_stats()


def head_forward(n, groups, factor, hidden, table, cluster, projs, weight):
    f32, bf16 = jnp.float32, jnp.bfloat16
    tokens, words = hidden.shape[0], weight.shape[1]
    capacity = tokens // 4
    size = projs[0].shape[1]
    rest = projs[1].shape[1] + projs[2].shape[1]
    wide = block_width(words, 256)
    vmem = pl.BlockSpec(memory_space=pltpu.VMEM)
    hbm = pl.BlockSpec(memory_space=pl.ANY)
    dma = pltpu.SemaphoreType.DMA
    return pl.pallas_call(
        functools.partial(head_kernel, n, groups, factor),
        out_shape=(
            jax.ShapeDtypeStruct((tokens, words), bf16),
            jax.ShapeDtypeStruct((capacity, rest), bf16),
            jax.ShapeDtypeStruct((capacity, rest), bf16),
            jax.ShapeDtypeStruct((capacity // n, size), f32),
            jax.ShapeDtypeStruct((tokens, 128), bf16),
            jax.ShapeDtypeStruct((tokens, 128), bf16),
            jax.ShapeDtypeStruct((8, tokens), f32),
            jax.ShapeDtypeStruct((8, 128), f32),
        ),
        in_specs=[vmem] * 6 + [hbm],
        out_specs=(vmem,) * 8,
        scratch_shapes=[
            pltpu.VMEM((2, weight.shape[0], wide), bf16),
            pltpu.VMEM((tokens, words), f32),
            pltpu.VMEM((tokens, 128), f32),
            pltpu.VMEM((tokens, 128), f32),
            pltpu.VMEM((n, 8, tokens), f32),
            pltpu.VMEM((tokens, 128), jnp.int32),
            pltpu.VMEM((capacity, size), f32),
            pltpu.VMEM((capacity, rest), f32),
            pltpu.VMEM((3 * capacity, tokens), bf16),
            pltpu.VMEM((groups, 8, 128), f32),
            dma((2,)),
            dma((n - 1,)),
            dma((n - 1,)),
            dma((groups - 1,)),
            dma((groups - 1,)),
        ]
        + scatter_scratch(n, capacity, size)
        + scatter_scratch(n, capacity, rest)
        + gather_scratch(n, capacity, rest),
        compiler_params=pltpu.CompilerParams(
            collective_id=1, has_side_effects=True, vmem_limit_bytes=60_000_000
        ),
    )(hidden, table, cluster, *projs, weight)


def ring_kernel(
    n,
    groups,
    factor,
    grad,
    table,
    high,
    low,
    chunk_one,
    cluster_high,
    cluster_low,
    cluster_rows,
    proj_one,
    proj_two,
    proj_three,
    weights,
    head_stats,
    weight,
    out_one,
    out_two,
    out_three,
    grads,
    losses,
    mean,
    blocks,
    ring,
    term,
    buf_one,
    buf_two,
    buf_three,
    mix,
    acc_one,
    acc_two,
    acc_three,
    sum_acc,
    pick_acc,
    stat_one,
    stat_rest,
    given_one,
    given_rest,
    high_one,
    low_one,
    aims,
    joins,
    backs,
    pair,
    tail_row,
    mean_all,
    block_sem,
    buf_sem,
    ring_send,
    ring_recv,
    stat_send,
    stat_recv,
    mean_send,
    mean_recv,
    *refs,
):
    f32, bf16 = jnp.float32, jnp.bfloat16
    me = lax.axis_index("vocab")
    half_n = n // 2
    odd = me % 2
    line = me // 2
    spot = (1 - odd) * line + odd * (n - 1 - line)

    def at(place):
        place = place % n
        back = place // half_n
        return (1 - back) * (2 * place) + back * (2 * (n - 1 - place) + 1)

    neighbour = (at(spot + 1), at(spot + n - 1))
    group = lax.axis_index("dp")
    barrier = greet(n, me, groups, group)
    width = blocks.shape[2]

    def block_copy(way, hop):
        place = at(spot + (n - 1 - hop if way == 0 else 1 + hop))
        start = pl.multiple_of(place * width, width)
        slot = hop % 2
        return pltpu.make_async_copy(
            weight.at[pl.ds(start, width), :], blocks.at[way, slot], block_sem.at[way, slot]
        )

    for hop in range(2):
        for way in range(2):
            block_copy(way, hop).start()

    capacity = high.shape[0]
    tokens = grad.shape[0]
    kinds = []
    size_two = out_two.shape[0]
    for number, (out, buf, acc, proj, tops, rests, given, span) in enumerate(
        (
            (out_one, buf_one, acc_one, proj_one, high_one, low_one, given_one, slice(None)),
            (out_two, buf_two, acc_two, proj_two, high, low, given_rest, slice(0, size_two)),
            (
                out_three,
                buf_three,
                acc_three,
                proj_three,
                high,
                low,
                given_rest,
                slice(size_two, high.shape[1]),
            ),
        )
    ):
        words = out.shape[1]
        wide = buf.shape[2]
        kinds.append(
            (number, span, out, buf, acc, words, wide, words // wide, proj, tops, rests, given)
        )

    def fetch(kind, i, slot):
        number, out, buf, wide = kind[0], kind[2], kind[3], kind[6]
        start = pl.multiple_of(i * wide, wide)
        source = out.at[:, pl.ds(start, wide)]
        if number < 2:
            return [pltpu.make_async_copy(source, buf.at[slot], buf_sem.at[number, slot])]
        size = out.shape[0]
        return [
            pltpu.make_async_copy(
                source, buf.at[slot, pl.ds(again * size, size), :], buf_sem.at[number + again, slot]
            )
            for again in range(2)
        ]

    for kind in kinds:
        for copy in fetch(kind, 0, 0):
            copy.start()
        acc = kind[4]
        acc[...] = jnp.zeros_like(acc)
    sum_acc[...] = jnp.zeros_like(sum_acc)
    pick_acc[...] = jnp.zeros_like(pick_acc)

    def tail_steps(kind, first, last):
        number, span, out, buf, acc, words, wide, count, _, tops, rests, _ = kind
        rows = pl.ds(number * capacity, capacity)

        def body(i, carry):
            slot = i % 2
            for copy in fetch(kind, i, slot):
                copy.wait()

            @pl.when(i + 1 < count)
            def _():
                for copy in fetch(kind, i + 1, 1 - slot):
                    copy.start()

            words_here = buf[slot]
            if number < 2:
                values = jnp.dot(tops[:, span], words_here, preferred_element_type=f32)
                values = values + jnp.dot(rests[:, span], words_here, preferred_element_type=f32)
            else:
                values = jnp.dot(pair[...], words_here, preferred_element_type=f32)
                words_here = buf[slot, 0 : acc.shape[1], :]
            aim = aims[rows, :] - me * words - i * wide
            total = sum_acc[rows, :]
            pick = pick_acc[rows, :]
            lane = lax.broadcasted_iota(jnp.int32, (capacity, 128), 1)
            for j in range(0, wide, 128):
                ratio = jnp.tanh(values[:, j : j + 128] * (1.0 / capping))
                power = jnp.exp2(ratio * (capping * LOG2E))
                hit = lane + j == aim
                total = total + power
                pick = pick + jnp.where(hit, ratio, 0.0)
                slope = 1.0 - ratio * ratio
                mix[0:capacity, j : j + 128] = jnp.where(hit, 0.0, power * slope).astype(bf16)
                mix[capacity : 2 * capacity, j : j + 128] = jnp.where(hit, 1.0, 0.0).astype(bf16)
            sum_acc[rows, :] = total
            pick_acc[rows, :] = pick
            acc[...] += dot_nt(mix[:, 0:wide], words_here)
            return carry

        lax.fori_loop(first, last, body, 0)

    one_stats = share_row(n, me, stat_one, stat_send.at[0], stat_recv.at[0])
    rest_stats = share_row(n, me, stat_rest, stat_send.at[1], stat_recv.at[1])
    latent_send, latent_swap, latent_take, latent_end = gather_phases(n, me, refs[0:5])
    one_half, one_spread, one_sum, one_drain = scatter_phases(n, me, given_one, refs[5:12])
    one_send, one_swap, one_take, one_end = gather_phases(n, me, refs[12:17])
    rest_half, rest_spread, rest_sum, rest_drain = scatter_phases(n, me, given_rest, refs[17:24])
    rest_send, rest_swap, rest_take, rest_end = gather_phases(n, me, refs[24:29])
    one, two, three = kinds

    def set_up():
        slot_row = table[2:3, :]
        target_row = table[1:2, :].astype(f32)
        for base in range(0, 3 * capacity, 128):
            slot = lax.broadcasted_iota(jnp.int32, (128, tokens), 0) + base
            found = jnp.where(slot == slot_row, target_row + 1.0, 0.0)
            found = jnp.sum(found, axis=1, keepdims=True) - 1.0
            aims[base : base + 128, :] = jnp.broadcast_to(found, (128, 128)).astype(jnp.int32)
        size = kinds[2][4].shape[1]
        pair[:, 0:size] = high[:, kinds[2][1]]
        pair[:, size : 2 * size] = low[:, kinds[2][1]]

    def join_slots():
        slots_here = spread_row(table[2:3, :])
        lanes = lax.broadcasted_iota(jnp.int32, (tokens, 128), 1)
        for base in range(0, 3 * capacity, 128):
            hit = lanes + base == slots_here
            joins[:, base : base + 128] = jnp.where(hit, 1.0, 0.0).astype(bf16)

    def take_latents():
        latent_take()
        high_one[...], low_one[...] = split_pair(refs[0][...])

    def share_stats(stats_of, first, last):
        rows = slice(first * capacity, last * capacity)
        stats_of[0](sum_acc[rows, :], capping * pick_acc[rows, :])

    def finish_stats(stats_of, group, send_half):
        whole = stats_of[1]()
        first = group[0][0]
        gap = jnp.log(whole[0:1, :]) - whole[1:2, :]
        for number, span, _, _, acc, words, _, _, _, _, _, given in group:
            rows = slice(number * capacity, (number + 1) * capacity)
            here = slice((number - first) * capacity, (number - first + 1) * capacity)
            total = column_of(whole[0:1, here])
            share = weights[number : number + 1, 0:1]
            tail_row[0:1, rows] = share * gap[:, here]
            ratio = jnp.sum(pick_acc[rows, :], axis=1, keepdims=True)
            pick = capping * ratio
            aim = aims[rows, 0:1]
            local = aim - me * words
            peak = (factor * (jnp.exp(pick) / total - 1.0) * (1.0 - ratio * ratio)).astype(bf16)
            inside = jnp.logical_and(local >= 0, local < words)
            peak = jnp.where(inside, peak.astype(f32), 0.0)
            scale = jnp.where(aim >= 0, factor / total, 0.0)
            given[:, span] = share * (
                scale * acc[0:capacity, :] + peak * acc[capacity : 2 * capacity, :]
            )
        send_half()

    def take_back(group, take, collected):
        take()
        for number, span, _, _, _, _, _, _, proj, _, _, _ in group:
            rows = slice(number * capacity, (number + 1) * capacity)
            top, lower = split_pair(collected[:, span])
            back = dot_nt(top, proj[...]) + dot_nt(lower, proj[...])
            backs[0, rows, :], backs[1, rows, :] = split_pair(back)

    send_mean, take_mean, drain_mean = share_groups(groups, group, mean_all, mean_send, mean_recv)

    def token_losses():
        tails = tail_row[0:1, :]
        total = jnp.zeros((tokens, 128), f32)
        for base in range(0, 3 * capacity, 128):
            total = total + joins[:, base : base + 128].astype(f32) * tails[:, base : base + 128]
        tail = jnp.sum(jnp.transpose(total), axis=0, keepdims=True)
        value = jnp.log(head_stats[0:1, :]) - head_stats[1:2, :] + tail
        losses[...] = jnp.broadcast_to(value, (8, tokens))
        send_mean(jnp.broadcast_to(jnp.sum(value, axis=1, keepdims=True), (8, 128)))

    def mean_loss():
        mean[...] = take_mean() * (1.0 / (groups * tokens))

    def join_backs():
        total = jnp.dot(joins[...], backs[0], preferred_element_type=f32)
        total = total + jnp.dot(joins[...], backs[1], preferred_element_type=f32)
        total = total + jnp.dot(cluster_high[...], cluster_rows[...], preferred_element_type=f32)
        grads[...] = total + jnp.dot(
            cluster_low[...], cluster_rows[...], preferred_element_type=f32
        )

    rows_way = grad.shape[0] // 2
    rows_part = rows_way // 2

    def product(way, hop):
        block_copy(way, hop).wait()
        part = grad[way * rows_way : (way + 1) * rows_way, :]
        return dot_nt(part, blocks[way, hop % 2])

    def products(hop):
        for way in range(2):
            block_copy(way, hop).wait()

        def body(way, carry):
            rows = pl.ds(pl.multiple_of(way * rows_way, rows_way), rows_way)
            term[way] = dot_nt(grad[rows, :], blocks[way, hop % 2])
            return carry

        lax.fori_loop(0, 2, body, 0)
        for way in range(2):
            next_block(way, hop)

    def next_block(way, hop):
        if hop + 2 < n:
            block_copy(way, hop + 2).start()

    def hop_copy(way, part, hop):
        rows = pl.ds(part * rows_part, rows_part)
        return peer_copy(
            ring.at[way, hop, rows, :],
            ring.at[way, hop + 1, rows, :],
            ring_send.at[way, part, hop],
            ring_recv.at[way, part, hop],
            neighbour[way],
        )

    def tails(kind, first, last):
        count = kind[7]
        return functools.partial(
            tail_steps, kind, int(count * first + 0.5), int(count * last + 0.5)
        )

    bind = functools.partial
    plan = [
        [set_up, tails(three, 0, 6 / 18)],
        [latent_swap, tails(three, 6 / 18, 12 / 18)],
        [tails(three, 12 / 18, 1)],
        [take_latents, tails(two, 0, 2 / 8)],
        [tails(two, 2 / 8, 1), bind(share_stats, rest_stats, 1, 3)],
        [bind(finish_stats, rest_stats, (two, three), rest_half), tails(one, 0, 2 / 4)],
        [rest_spread, tails(one, 2 / 4, 1), bind(share_stats, one_stats, 0, 1)],
        [
            bind(finish_stats, one_stats, (one,), one_half),
            lambda: rest_send(rest_sum()),
        ],
        [one_spread, rest_swap, join_slots, token_losses],
        [lambda: one_send(one_sum()), bind(take_back, (two, three), rest_take, refs[24])],
        [one_swap, mean_loss],
        [bind(take_back, (one,), one_take, refs[12]), join_backs],
    ]
    work = [[] for _ in range(2 * (n - 1))]
    for i, group in enumerate(plan):
        work[i * (len(work) - 2) // len(plan)] += group

    pl.semaphore_wait(barrier, n + groups - 2)
    for way in range(2):
        ring[way, 0] = product(way, 0)
        next_block(way, 0)
        for part in range(2):
            hop_copy(way, part, 0).start()
    latent_send(chunk_one[...])
    products(1)
    for hop in range(n - 1):
        for part in range(2):
            rows = pl.ds(part * rows_part, rows_part)
            for way in range(2):
                hop_copy(way, part, hop).wait_recv()
                held = ring[way, hop + 1, rows, :] + term[way, rows, :]
                if hop < n - 2:
                    ring[way, hop + 1, rows, :] = held
                    hop_copy(way, part, hop + 1).start()
                else:
                    grads[pl.ds(way * rows_way + part * rows_part, rows_part), :] += held
            if part == 1 and hop < n - 2:
                products(hop + 2)
            for piece in work[2 * hop + part]:
                piece()
    for way in range(2):
        for part in range(2):
            for hop in range(n - 1):
                hop_copy(way, part, hop).wait_send()
    one_stats[2]()
    rest_stats[2]()
    drain_mean()
    latent_end()
    one_drain()
    one_end()
    rest_drain()
    rest_end()


def ring_and_tails(
    n, groups, factor, grad, table, latents, clusters, projs, weights, head_stats, weight, outs
):
    f32, bf16 = jnp.float32, jnp.bfloat16
    tokens = grad.shape[0]
    capacity = latents[0].shape[0]
    width = projs[0].shape[0]
    rest = latents[0].shape[1]
    sizes = [out.shape[0] for out in outs]
    wides = [block_width(out.shape[1], 1024) for out in outs]
    vmem = pl.BlockSpec(memory_space=pltpu.VMEM)
    hbm = pl.BlockSpec(memory_space=pl.ANY)
    dma = pltpu.SemaphoreType.DMA
    return pl.pallas_call(
        functools.partial(ring_kernel, n, groups, factor),
        out_shape=(
            jax.ShapeDtypeStruct((tokens, width), f32),
            jax.ShapeDtypeStruct((8, tokens), f32),
            jax.ShapeDtypeStruct((8, 128), f32),
        ),
        in_specs=[vmem] * 13 + [hbm] * 4,
        out_specs=(vmem, vmem, vmem),
        scratch_shapes=[
            pltpu.VMEM((2, 2, width, weight.shape[1]), bf16),
            pltpu.VMEM((2, n, tokens // 2, width), f32),
            pltpu.VMEM((2, tokens // 2, width), f32),
        ]
        + [
            pltpu.VMEM((2, times * size, wide), bf16)
            for times, size, wide in zip((1, 1, 2), sizes, wides)
        ]
        + [pltpu.VMEM((2 * capacity, max(wides)), bf16)]
        + [pltpu.VMEM((2 * capacity, size), f32) for size in sizes]
        + [
            pltpu.VMEM((3 * capacity, 128), f32),
            pltpu.VMEM((3 * capacity, 128), f32),
            pltpu.VMEM((n, 8, capacity), f32),
            pltpu.VMEM((n, 8, 2 * capacity), f32),
            pltpu.VMEM((capacity, sizes[0]), f32),
            pltpu.VMEM((capacity, rest), f32),
            pltpu.VMEM((capacity, sizes[0]), bf16),
            pltpu.VMEM((capacity, sizes[0]), bf16),
            pltpu.VMEM((3 * capacity, 128), jnp.int32),
            pltpu.VMEM((tokens, 3 * capacity), bf16),
            pltpu.VMEM((2, 3 * capacity, width), bf16),
            pltpu.VMEM((capacity, 2 * sizes[2]), bf16),
            pltpu.VMEM((8, 3 * capacity), f32),
            pltpu.VMEM((groups, 8, 128), f32),
            dma((2, 2)),
            dma((4, 2)),
            dma((2, 2, n - 1)),
            dma((2, 2, n - 1)),
            dma((2, n - 1)),
            dma((2, n - 1)),
            dma((groups - 1,)),
            dma((groups - 1,)),
        ]
        + gather_scratch(n, capacity, sizes[0])
        + scatter_scratch(n, capacity, sizes[0])
        + gather_scratch(n, capacity, sizes[0])
        + scatter_scratch(n, capacity, rest)
        + gather_scratch(n, capacity, rest),
        compiler_params=pltpu.CompilerParams(
            collective_id=0, has_side_effects=True, vmem_limit_bytes=66_000_000
        ),
    )(grad, table, *latents, *clusters, *projs, weights, head_stats, weight, *outs)


def per_device(
    n,
    groups,
    hidden,
    labels,
    targets,
    head_weight,
    cluster_weight,
    proj_one,
    proj_two,
    proj_three,
    out_one,
    out_two,
    out_three,
):
    f32, bf16 = jnp.float32, jnp.bfloat16
    tokens = hidden.shape[0]
    width = proj_one.shape[0]
    head_local = head_weight.shape[1]
    capacity = tokens // 4
    all_tokens = tokens * groups
    vocab_index = lax.axis_index("vocab")
    feat_start = vocab_index * width
    factor = jnp.sqrt(f32(hidden.shape[1]))
    projs = (proj_one, proj_two, proj_three)
    outs = (out_one, out_two, out_three)

    member = labels[None, :] == jnp.arange(1, 4, dtype=jnp.int32)[:, None]
    local_counts = jnp.sum(member.astype(f32), 1)
    row = jnp.arange(tokens, dtype=jnp.int32)
    upto = (row[:, None] <= row[None, :]).astype(bf16)
    placed = jnp.dot(member.astype(bf16), upto, preferred_element_type=f32).astype(jnp.int32) - 1
    offsets = jnp.arange(3, dtype=jnp.int32)[:, None] * capacity
    slot_of = jnp.sum(jnp.where(member, placed + offsets + 1, 0), 0) - 1
    slot_ids = jnp.arange(3 * capacity, dtype=jnp.int32)
    chosen = slot_ids[:, None] == slot_of[None, :]
    select = chosen.astype(bf16)
    slot_aims = jnp.sum(jnp.where(chosen, targets[None, :] + 1, 0), 1) - 1
    filled = (slot_aims >= 0).astype(f32)

    own_features = lax.dynamic_slice_in_dim(hidden, feat_start, width, 1)
    picked_rows = jnp.dot(select, own_features, preferred_element_type=f32).astype(bf16)
    latent_parts = []
    for number in range(3):
        chunk = picked_rows[number * capacity : (number + 1) * capacity]
        latent_parts.append(jnp.dot(chunk, projs[number], preferred_element_type=f32))
    counts = butterfly_sum(local_counts, "dp", groups)
    weights = all_tokens / (4.0 * counts)
    clus_cap = capped(jnp.dot(hidden, cluster_weight, preferred_element_type=f32))
    clus_exp = jnp.exp(clus_cap)
    clus_hit = (jnp.arange(3, dtype=jnp.int32)[None, :] + 1 == labels[:, None]).astype(f32)
    clus_sum = jnp.sum(clus_exp, 1)
    clus_slope = 1.0 - (clus_cap * (1.0 / capping)) ** 2
    head_aims = jnp.where(labels == 0, targets, -1) - vocab_index * head_local
    clus_rows = lax.dynamic_slice_in_dim(cluster_weight, feat_start, width, 0)

    if n <= RING_LIMIT:
        scale_of = float(hidden.shape[1]) ** 0.5
        table = jnp.concatenate(
            [
                jnp.stack([labels, targets, slot_of]),
                jnp.zeros((5, tokens), jnp.int32),
            ],
            0,
        )
        padded = jnp.pad(cluster_weight, ((0, 0), (0, 125)))
        grad, high, low, chunk, clus_high, clus_low, head_stats, weights = head_forward(
            n, groups, scale_of, hidden, table, padded, projs, head_weight
        )
        clus_lines = jnp.pad(jnp.transpose(clus_rows), ((0, 125), (0, 0)))
        grads, losses, mean = ring_and_tails(
            n,
            groups,
            scale_of,
            grad,
            table,
            (high, low, chunk),
            (clus_high, clus_low, clus_lines),
            projs,
            weights,
            head_stats,
            head_weight,
            outs,
        )
        return (losses[0], mean[0, 0], grads)
    else:
        powers = []
        step = 1
        while step < n:
            powers.append(step)
            step *= 2
        turned = powers[1:] + powers[:1]
        joined = jnp.concatenate([latent_parts[1], latent_parts[2]], 1)
        joined = halving_sum(joined, "vocab", n, turned)
        width_two = projs[1].shape[1]
        latents = [
            halving_sum(latent_parts[0], "vocab", n, powers),
            joined[:, :width_two],
            joined[:, width_two:],
        ]
        head_cap = capped(jnp.dot(hidden, head_weight, preferred_element_type=f32))
        head_sum = jnp.sum(jnp.exp(head_cap), 1)
        head_sum = butterfly_sum(head_sum, "vocab", n)
        head_hit = jnp.arange(head_local, dtype=jnp.int32)[None, :] == head_aims[:, None]
        total = head_sum + clus_sum
        scale = factor / total
        kept_cap = lax.optimization_barrier(head_cap)
        head_pick = jnp.sum(jnp.where(head_hit, kept_cap, 0.0), 1)
        slope = 1.0 - (kept_cap * (1.0 / capping)) ** 2
        head_grad = (
            (jnp.exp(kept_cap) * scale[:, None] - jnp.where(head_hit, factor, 0.0)) * slope
        ).astype(bf16)
        clus_grad = (clus_exp * scale[:, None] - factor * clus_hit) * clus_slope
        head_terms = jnp.einsum("tv,fv->tf", head_grad, head_weight, preferred_element_type=f32)
        head_back = lax.psum_scatter(head_terms, "vocab", scatter_dimension=1, tiled=True)

        tail_caps, tail_hits, tail_sums, tail_picks = [None] * 3, [None] * 3, [None] * 3, [None] * 3
        for number in (1, 2, 0):
            out = outs[number]
            tail_cap = capped(
                jnp.dot(latents[number], out.astype(f32), precision=lax.Precision.HIGH)
            )
            aims = slot_aims[number * capacity : (number + 1) * capacity]
            aims = jnp.where(aims >= 0, aims, -1) - vocab_index * out.shape[1]
            aims = jnp.where(slot_aims[number * capacity : (number + 1) * capacity] >= 0, aims, -1)
            tail_hits[number] = jnp.arange(out.shape[1], dtype=jnp.int32)[None, :] == aims[:, None]
            tail_sums[number] = jnp.sum(jnp.exp(tail_cap), 1)
            tail_caps[number] = lax.optimization_barrier(tail_cap)
            tail_picks[number] = jnp.sum(jnp.where(tail_hits[number], tail_caps[number], 0.0), 1)
        tail_totals = butterfly_sum(jnp.concatenate(tail_sums), "vocab", n)
        tail_scales = factor * filled / tail_totals
        grad_parts = [None] * 3
        for number in (0, 1, 2):
            cap = tail_caps[number]
            tail_scale = tail_scales[number * capacity : (number + 1) * capacity]
            tail_grad = (
                (jnp.exp(cap) * tail_scale[:, None] - jnp.where(tail_hits[number], factor, 0.0))
                * (1.0 - (cap * (1.0 / capping)) ** 2)
            ).astype(bf16)
            grad_parts[number] = jnp.einsum(
                "sv,pv->sp", tail_grad, outs[number], preferred_element_type=f32
            )
        grad_one = halving_sum(grad_parts[0], "vocab", n, powers)
        grad_rest = halving_sum(jnp.concatenate([grad_parts[1], grad_parts[2]], 1), "vocab", n, turned)
        latent_grads = [grad_one, grad_rest[:, :width_two], grad_rest[:, width_two:]]
        tail_picks = butterfly_sum(jnp.concatenate(tail_picks), "vocab", n)

        backs = []
        for number in range(3):
            back = jnp.einsum(
                "sp,fp->sf",
                latent_grads[number],
                projs[number].astype(f32),
                precision=lax.Precision.HIGH,
            )
            backs.append(weights[number] * back)
        back = jnp.concatenate(backs, 0)
        back_top = lax.reduce_precision(back, 8, 7)
        back_rest = (back - back_top).astype(bf16)
        back_top = back_top.astype(bf16)
        pick_slots = functools.partial(jnp.einsum, "st,sf->tf", preferred_element_type=f32)
        tail_back = pick_slots(select, back_top) + pick_slots(select, back_rest)
        clus_rows = clus_rows.astype(f32)
        clus_back = (
            clus_grad[:, 0:1] * clus_rows[:, 0][None, :]
            + clus_grad[:, 1:2] * clus_rows[:, 1][None, :]
            + clus_grad[:, 2:3] * clus_rows[:, 2][None, :]
        )
        grads = head_back + (tail_back + clus_back)
        head_pick = butterfly_sum(head_pick, "vocab", n)
        head_loss = jnp.log(total) - head_pick - jnp.sum(clus_hit * clus_cap, 1)

    tail_loss = (jnp.log(tail_totals) - tail_picks) * filled
    slot_weights = jnp.repeat(weights, capacity)
    tail_loss = tail_loss * slot_weights
    token_loss = head_loss + jnp.sum(jnp.where(chosen, tail_loss[:, None], 0.0), 0)
    loss_sum = butterfly_sum(jnp.sum(token_loss)[None], "dp", groups)
    mean_loss = loss_sum[0] / all_tokens
    return (token_loss, mean_loss, grads)


def solution(mesh):
    body = functools.partial(per_device, mesh.shape["vocab"], mesh.shape["dp"])
    return jax.shard_map(
        body,
        mesh=mesh,
        in_specs=(
            P("dp", None),
            P("dp"),
            P("dp"),
            P(None, "vocab"),
            P(),
            P("vocab", None),
            P("vocab", None),
            P("vocab", None),
            P(None, "vocab"),
            P(None, "vocab"),
            P(None, "vocab"),
        ),
        out_specs=(P("dp"), P(), P("dp", "vocab")),
        check_vma=False,
    )
```
